32 devices in a mesh: dp: 4 (over y, x), expert: 4 (over z), tensor: 2 (over core).
Axes of the slice: x: 2, y: 2, z: 4, core: 2. Of those that a mesh axis runs over, the one named last changes fastest.
Arguments:
- tokens: bfloat16 [2048, 2560], P(('dp', 'expert')), may hold values from -6 to 6
- norm_gain: float32 [2560], replicated, may hold values from 0.5 to 1.5
- expert_ids: int32 [2048, 6], P(('dp', 'expert')), may hold values from 0 to 31, all different within a row; in each aligned block of 128 rows (0 to 127, 128 to 255, ...) at most 48 rows name the same one
- route_weights: int32 [2048, 6], P(('dp', 'expert')), may hold values from 1 to 64
- w_gate: bfloat16 [32, 2560, 768], P('expert', None, 'tensor'), may hold values from -0.125 to 0.125
- w_up: bfloat16 [32, 2560, 768], P('expert', None, 'tensor'), may hold values from -0.125 to 0.125
- w_down: bfloat16 [32, 768, 2560], P('expert', 'tensor'), may hold values from -0.21875 to 0.21875
- shared_gate: bfloat16 [2560, 2048], P(None, ('dp', 'tensor')), may hold values from -0.125 to 0.125
- shared_up: bfloat16 [2560, 2048], P(None, ('dp', 'tensor')), may hold values from -0.125 to 0.125
- shared_down: bfloat16 [2048, 2560], P(('dp', 'tensor')), may hold values from -0.125 to 0.125
Outputs:
- mixed: bfloat16 [2048, 2560], P(('dp', 'expert'), 'tensor')
The draws below stay inside these ranges and needn't reach their ends.
Inputs may be any that keep to these rules, and one draw needn't show every extreme that they name: `expert_ids`: each row names 6 different experts. In each aligned block of 128 rows (the rows of one index of dp+expert) no expert is named by more than 48 rows, a bound that some blocks reach.
All inputs are finite; a program needn't handle non-finite values.
Results may differ from the reference program's by a relative error of at most 0.011.
Values may be sent and summed in bfloat16 or wider, within the bound.
A program may use at most 128 MiB of HBM per device.

```python
import math
import jax
import jax.numpy as jnp
import numpy as np
from jax import lax

D = 2560
FF = 768
SFF = 2048
EXPERTS = 32
TOP = 6
TOK_DEV = 128
CAP = 48
TOKENS = 2048


def place_ends(values, own_key, low, largest):
    spot = [jax.random.randint(jax.random.fold_in(own_key, axis), (), 0, length) for axis, length in enumerate(values.shape)]
    widest = values.shape.index(max(values.shape))
    next_to = spot[:widest] + [(spot[widest] + 1) % values.shape[widest]] + spot[widest + 1:]
    return values.at[tuple(spot)].set(low).at[tuple(next_to)].set(largest)


def shard_levels(rng, extent, split, low, largest):
    loudness = 1.0
    for dim, parts in split:
        draws = jax.random.uniform(jax.random.fold_in(jax.random.fold_in(rng, 6), dim), (parts,), jnp.float32, low / len(split), largest / len(split))
        loudness = loudness * jnp.repeat(jnp.exp(draws), extent[dim] // parts).reshape((-1,) + (1,) * (len(extent) - 1 - dim))
    return loudness


def deal_out(key, own, number, rows, number_of, top, reach, slope):
    ranking = jax.random.permutation(key, number_of)
    crowded, usual = portions_of(number_of, rows * top, reach, slope, True), portions_of(number_of, rows * top, reach, slope, False)
    places = jnp.arange(number_of)

    def named(tallies, offset_by):
        used = int((tallies > 0).sum())
        fixed = max(1, used // 4)
        shifted = fixed + (places - fixed + offset_by * (used - fixed)) % max(1, number_of - fixed)
        return jnp.zeros((number_of,), jnp.int32).at[ranking[jnp.where(places < fixed, places, shifted)]].set(jnp.asarray(tallies, jnp.int32))

    tallies = jnp.where(number % 4 == 0, named(crowded, number // 4), named(usual, number - number // 4 - 1))
    mixed = jax.random.permutation(jax.random.fold_in(own, 3), number_of)
    donor, taker = mixed[0:number_of // 2 * 2:2], mixed[1:number_of // 2 * 2:2]
    slack = jnp.minimum(tallies[donor] - 1, reach - tallies[taker]) // 2
    slack = jnp.where((donor == ranking[0]) | (taker == ranking[0]) | (tallies[taker] == 0), 0, jnp.maximum(slack, 0))
    shifted = jax.random.randint(jax.random.fold_in(own, 4), (number_of // 2,), 0, 1 << 20) % (slack + 1)
    tallies = tallies.at[donor].add(-shifted).at[taker].add(shifted)
    labels = jnp.searchsorted(jnp.cumsum(tallies), jnp.arange(rows * top), side="right").astype(jnp.int32)
    table = labels.reshape(top, rows).T
    table = table[jax.random.permutation(jax.random.fold_in(own, 1), rows)]
    offset_by = jax.random.randint(jax.random.fold_in(own, 2), (rows, 1), 0, top)
    return jnp.take_along_axis(table, (jnp.arange(top)[None, :] + offset_by) % top, axis=1)


def portions_of(count, total, limit, skew, full):
    portions = [(1 << 20) // math.isqrt(standing ** skew) + 1 for standing in range(1, count + 1)]
    largest = limit if full else min(limit, max(-(-total // count), total * portions[0] // sum(portions)))
    least = 1 if total - largest >= count - 1 else 0
    holding, rest = [largest] + [least] * (count - 1), total - largest - least * (count - 1)
    while rest > 0:
        movable = [i for i in range(1, count) if holding[i] < largest] or [i for i in range(1, count) if holding[i] < limit]
        pool, left = sum([portions[i] for i in movable]), rest
        for i in movable:
            extra = min(limit - holding[i], max(1, left * portions[i] // pool), rest)
            holding[i] = holding[i] + extra
            rest = rest - extra
    return np.array(holding)


def bell_draw(rng, dims, deviation, bound, cuts=(), kind=jnp.bfloat16):
    values = jax.random.normal(rng, dims, jnp.float32) * deviation
    if len(cuts) > 0:
        values = shard_levels(rng, dims, cuts, -0.22, 0.18) * values
    return jnp.clip(values, min=-bound, max=bound).astype(kind)


def setup_inputs(seed: int = 0) -> dict:
    keys = jax.random.split(jax.random.key(seed), 11)
    tokens = bell_draw(keys[0], (TOKENS, D), 1.0, 6.0, ((0, 16),))
    norm_gain = jnp.clip(1.0 + 0.1 * jax.random.normal(keys[1], (D,), jnp.float32), 0.5, 1.5)
    expert_ids_keys = jax.random.split(jax.random.fold_in(keys[2], 1), TOKENS // TOK_DEV)
    expert_ids_turns = jax.random.permutation(jax.random.fold_in(keys[2], 3), TOKENS // TOK_DEV)
    expert_ids = jax.vmap(lambda own, number: deal_out(jax.random.fold_in(keys[2], 2), own, number, TOK_DEV, EXPERTS, TOP, CAP, 2))(expert_ids_keys, expert_ids_turns).reshape((TOKENS, TOP))
    route_weights = place_ends(jax.random.randint(keys[3], (TOKENS, TOP), 1, 65), jax.random.fold_in(keys[3], 1), 1, 64).astype(jnp.int32)
    w_gate = bell_draw(keys[4], (EXPERTS, D, FF), D ** -0.5, 0.125, ((0, 4), (2, 2)))
    w_up = bell_draw(keys[5], (EXPERTS, D, FF), D ** -0.5, 0.125, ((0, 4), (2, 2)))
    w_down = bell_draw(keys[6], (EXPERTS, FF, D), FF ** -0.5, 0.21875, ((0, 4), (1, 2)))
    shared_gate = bell_draw(keys[7], (D, SFF), D ** -0.5, 0.125, ((1, 8),))
    shared_up = bell_draw(keys[8], (D, SFF), D ** -0.5, 0.125, ((1, 8),))
    shared_down = bell_draw(keys[9], (SFF, D), SFF ** -0.5, 0.125, ((0, 8),))
    return {"tokens": tokens, "norm_gain": norm_gain, "expert_ids": expert_ids, "route_weights": route_weights, "w_gate": w_gate, "w_up": w_up, "w_down": w_down, "shared_gate": shared_gate, "shared_up": shared_up, "shared_down": shared_down}


EPSILON = 1e-06

def normalize(tokens, norm_gain):
    values = tokens.astype(jnp.float32)
    inverse = lax.rsqrt(lax.optimization_barrier(jnp.mean(values * values, axis=1, keepdims=True)) + EPSILON)
    return (values * inverse * norm_gain.astype(jnp.float32)[None, :]).astype(jnp.bfloat16)

def reference(tokens, norm_gain, expert_ids, route_weights, w_gate, w_up, w_down, shared_gate, shared_up, shared_down):
    normed = normalize(tokens, norm_gain)
    groups = TOKENS // TOK_DEV
    pair_total = TOK_DEV * TOP
    local_ids = expert_ids.reshape(groups, pair_total).astype(jnp.int32)
    onehot = (local_ids[:, :, None] == jnp.arange(EXPERTS, dtype=jnp.int32)[None, None, :]).astype(jnp.int32)
    earlier = jnp.cumsum(onehot, axis=1) - onehot
    slot_index = lax.optimization_barrier(jnp.sum(earlier * onehot, axis=2)).astype(jnp.int32)
    position = (local_ids * CAP + slot_index).astype(jnp.int32)
    group_index = jnp.broadcast_to(jnp.arange(groups, dtype=jnp.int32)[:, None], (groups, pair_total)).astype(jnp.int32)
    pair_token = (group_index * TOK_DEV + jnp.arange(pair_total, dtype=jnp.int32)[None, :] // TOP).astype(jnp.int32)
    filler = jnp.full((groups, EXPERTS * CAP), -1, jnp.int32).at[group_index, position].set(pair_token)
    pair_scale = route_weights.astype(jnp.float32).reshape(groups, pair_total) / 64.0
    slot_scale = jnp.zeros((groups, EXPERTS * CAP), jnp.float32).at[group_index, position].set(pair_scale)
    filler = filler.reshape(groups, EXPERTS, CAP).transpose(1, 0, 2).reshape(EXPERTS, groups * CAP)
    slot_scale = slot_scale.reshape(groups, EXPERTS, CAP).transpose(1, 0, 2).reshape(EXPERTS, groups * CAP)

    def expert_step(totals, inputs):
        owner_rows, owner_scale, gate_weight, up_weight, down_weight = inputs
        valid = owner_rows >= 0
        safe_rows = jnp.maximum(owner_rows, 0).astype(jnp.int32)
        picked = jnp.where(valid[:, None], normed[safe_rows], jnp.zeros((), jnp.bfloat16))
        gate_value = jnp.dot(picked, gate_weight, preferred_element_type=jnp.float32)
        up_value = jnp.dot(picked, up_weight, preferred_element_type=jnp.float32)
        hidden = (jax.nn.silu(gate_value) * up_value).astype(jnp.bfloat16)
        result = jnp.dot(hidden, down_weight, preferred_element_type=jnp.float32).astype(jnp.bfloat16)
        update = result.astype(jnp.float32) * owner_scale[:, None]
        update = jnp.where(valid[:, None], update, jnp.zeros((), jnp.float32))
        return (totals.at[safe_rows].add(update), None)
    routed, unused = lax.scan(expert_step, jnp.zeros((TOKENS, D), jnp.float32), (filler, slot_scale, w_gate, w_up, w_down))
    shared_gate_value = jnp.dot(normed, shared_gate, preferred_element_type=jnp.float32)
    shared_up_value = jnp.dot(normed, shared_up, preferred_element_type=jnp.float32)
    shared_hidden = (jax.nn.silu(shared_gate_value) * shared_up_value).astype(jnp.bfloat16)
    shared_out = jnp.dot(shared_hidden, shared_down, preferred_element_type=jnp.float32)
    return (shared_out + routed).astype(jnp.bfloat16)
```

```python
import functools

import jax
import jax.numpy as jnp
from jax import lax
from jax.experimental import pallas as pl
from jax.experimental.pallas import tpu as pltpu
from jax.sharding import PartitionSpec as P

EPSILON = 1e-06
LANES = 128
PIECES = 2
MESH = pl.DeviceIdType.MESH
VMEM_BYTES = 67043328


def dot(a, b):
    return jnp.dot(a, b, preferred_element_type=jnp.float32)


def silu(v):
    return v / (1.0 + jnp.exp(-v))


def kernel(
    owners,
    groups,
    tokens,
    gain_in,
    ids_in,
    weights_in,
    w_gate,
    w_up,
    w_down,
    shared_gate,
    shared_up,
    shared_down,
    out,
    blocks,
    scales,
    peers,
    gate_up,
    down,
    shared_in,
    shared_out,
    hidden,
    shared_hidden,
    staged,
    shared_staged,
    keep,
    total,
    partner_routed,
    partner_shared,
    landed,
    gain,
    ids,
    weights,
    load_sem,
    shared_sem,
    token_sem,
    small_sem,
    zsend,
    zrecv,
    ssend,
    srecv,
    gsend,
    grecv,
    fsend,
    frecv,
    psend,
    precv,
    esend,
    erecv,
    xsend,
    xrecv,
    rsend,
    rrecv,
    qsend,
    qrecv,
):
    g = lax.axis_index("dp")
    z = lax.axis_index("expert")
    c = lax.axis_index("tensor")
    other = 1 - c
    local, ff, width = w_down.shape
    sff = shared_down.shape[0]
    rows = tokens.shape[0]
    half = width // 2
    experts = local * owners
    share = rows // 2
    piece = share // PIECES
    f32, bf16 = jnp.float32, jnp.bfloat16
    cut = -(-half // 512) * 256
    parts = ((0, cut), (cut, half - cut))

    def rows_of(core, k):
        return pl.ds(pl.multiple_of(core * share + k * piece, piece), piece)

    token_loads = [
        pltpu.make_async_copy(
            tokens.at[pl.ds(pl.multiple_of(core * share, share), share)],
            blocks.at[z, pl.ds(pl.multiple_of(core * share, share), share)],
            token_sem.at[p],
        )
        for p, core in enumerate((c, other))
    ]
    small_loads = [
        pltpu.make_async_copy(gain_in, gain, small_sem.at[0]),
        pltpu.make_async_copy(ids_in, ids, small_sem.at[1]),
        pltpu.make_async_copy(weights_in, weights, small_sem.at[2]),
    ]
    for load in token_loads + small_loads:
        load.start()

    def expert_loads(e):
        first = pl.ds(pl.multiple_of(e * ff, LANES), ff)
        return (
            pltpu.make_async_copy(w_gate.at[e], gate_up.at[e, :, pl.ds(0, ff)], load_sem.at[0, e]),
            pltpu.make_async_copy(w_up.at[e], gate_up.at[e, :, pl.ds(ff, ff)], load_sem.at[1, e]),
            pltpu.make_async_copy(w_down.at[e], down.at[first], load_sem.at[2, e]),
        )

    shared_loads = (
        pltpu.make_async_copy(shared_gate, shared_in.at[:, pl.ds(0, sff)], shared_sem.at[0]),
        pltpu.make_async_copy(shared_up, shared_in.at[:, pl.ds(sff, sff)], shared_sem.at[1]),
        pltpu.make_async_copy(shared_down, shared_out, shared_sem.at[2]),
    )

    barrier = pltpu.get_barrier_semaphore()
    for r in range(1, owners):
        peer = {"expert": lax.rem(z + r, owners)}
        pl.semaphore_signal(barrier, inc=1, device_id=peer, device_id_type=MESH)
    for r in range(1, groups):
        peer = {"dp": lax.rem(g + r, groups)}
        pl.semaphore_signal(barrier, inc=1, device_id=peer, device_id_type=MESH)
    pl.semaphore_signal(barrier, inc=1, device_id={"tensor": other}, device_id_type=MESH)

    for e in range(local):
        expert_loads(e)[0].start()
        expert_loads(e)[1].start()
    shared_loads[0].start()
    shared_loads[1].start()
    for e in range(local):
        expert_loads(e)[2].start()
    shared_loads[2].start()

    for load in small_loads:
        load.wait()
    lane_expert = lax.broadcasted_iota(jnp.int32, (experts, rows), 0)
    scale = jnp.zeros((experts, rows), f32)
    for k in range(ids.shape[0]):
        weight = weights[k : k + 1, :].astype(f32) * (1.0 / 64.0)
        scale = scale + jnp.where(ids[k : k + 1, :] == lane_expert, weight, 0.0)
    scales[z] = scale

    step = 16

    def norm(core):
        def body(t, carry):
            span = pl.ds(pl.multiple_of(core * share + t * step, step), step)
            value = blocks[z, span, :].astype(f32)
            square = jnp.sum(value * value, axis=1, keepdims=True)
            inverse = lax.rsqrt(square / width + EPSILON)
            blocks[z, span, :] = (value * inverse * gain[...]).astype(bf16)
            return carry

        lax.fori_loop(0, share // step, body, 0)

    def piece_send(b, k, way):
        return pltpu.make_async_remote_copy(
            src_ref=blocks.at[b, rows_of(c, k)],
            dst_ref=blocks.at[b, rows_of(c, k)],
            send_sem=zsend.at[way, b, k],
            recv_sem=zrecv.at[b, k],
            device_id={"expert": lax.rem(z + (1 if way else owners - 1), owners)},
            device_id_type=MESH,
        )

    def scale_send(b, way):
        return pltpu.make_async_remote_copy(
            src_ref=scales.at[b],
            dst_ref=scales.at[b],
            send_sem=ssend.at[way, b],
            recv_sem=srecv.at[b],
            device_id={"expert": lax.rem(z + (1 if way else owners - 1), owners)},
            device_id_type=MESH,
        )

    pairs = groups // 2 if groups % 2 == 0 else groups
    lows = groups // pairs

    def mate(k, sign):
        high, low = k // lows, k % lows
        up = lax.rem(g // lows + (high if sign > 0 else pairs - high), pairs)
        return up * lows + lax.rem(lax.rem(g, lows) + (low if sign > 0 else lows - low), lows)

    def peer_send(k):
        mine = pl.ds(pl.multiple_of(c * share, share), share)
        return pltpu.make_async_remote_copy(
            src_ref=blocks.at[z, mine],
            dst_ref=peers.at[k - 1, mine],
            send_sem=gsend.at[k - 1],
            recv_sem=grecv.at[k - 1],
            device_id={"dp": mate(k, 1)},
            device_id_type=MESH,
        )

    def pass_piece(b, k, core):
        return pltpu.make_async_remote_copy(
            src_ref=blocks.at[b, rows_of(core, k)],
            dst_ref=blocks.at[b, rows_of(core, k)],
            send_sem=fsend.at[b, k],
            recv_sem=frecv.at[b, k],
            device_id={"tensor": other},
            device_id_type=MESH,
        )

    def pass_peer(k, core):
        span = pl.ds(pl.multiple_of(core * share, share), share)
        return pltpu.make_async_remote_copy(
            src_ref=peers.at[k - 1, span],
            dst_ref=peers.at[k - 1, span],
            send_sem=psend.at[k - 1],
            recv_sem=precv.at[k - 1],
            device_id={"tensor": other},
            device_id_type=MESH,
        )

    def exchange(i, p):
        at = pl.ds(*parts[p])
        return pltpu.make_async_remote_copy(
            src_ref=staged.at[:, at],
            dst_ref=partner_routed.at[i, :, at],
            send_sem=esend.at[i, p],
            recv_sem=erecv.at[i, p],
            device_id={"tensor": other},
            device_id_type=MESH,
        )

    def result_send(i, p, slot, b):
        at = pl.ds(*parts[p])
        return pltpu.make_async_remote_copy(
            src_ref=partner_routed.at[i, :, at],
            dst_ref=landed.at[slot, :, at],
            send_sem=rsend.at[slot, p],
            recv_sem=rrecv.at[slot, p],
            device_id={"expert": b},
            device_id_type=MESH,
        )

    def shared_exchange(j):
        return pltpu.make_async_remote_copy(
            src_ref=shared_staged.at[j - 1],
            dst_ref=partner_shared.at[j - 1],
            send_sem=xsend.at[j - 1],
            recv_sem=xrecv.at[j - 1],
            device_id={"tensor": other},
            device_id_type=MESH,
        )

    def shared_result(j):
        return pltpu.make_async_remote_copy(
            src_ref=partner_shared.at[j - 1],
            dst_ref=landed.at[owners - 1 + j - 1],
            send_sem=qsend.at[j - 1],
            recv_sem=qrecv.at[j - 1],
            device_id={"dp": mate(j, -1)},
            device_id_type=MESH,
        )

    token_loads[0].wait()
    norm(c)
    pl.semaphore_wait(barrier, owners + groups - 1)

    def when(condition, action):
        @pl.when(condition)
        def _():
            action()

    def send_on(b, k, way):
        piece_send(b, k, way).start()
        if k == 0:
            scale_send(b, way).start()

    for k in range(PIECES):
        when(z + 1 < owners, lambda: send_on(z, k, 1))
        when(z > 0, lambda: send_on(z, k, 0))
    for k in range(1, groups):
        peer_send(k).start()

    token_loads[1].wait()
    norm(other)

    def arrive(b, k):
        here = blocks.at[b, rows_of(c, k)]
        pltpu.make_async_copy(here, here, zrecv.at[b, k]).wait()
        if k == 0:
            pltpu.make_async_copy(scales.at[b], scales.at[b], srecv.at[b]).wait()

    def fetch(d, k):
        @pl.when(z - d >= 0)
        def _():
            arrive(z - d, k)
            when(z + 1 < owners, lambda: send_on(z - d, k, 1))
            pass_piece(z - d, k, c).start()

        @pl.when(z + d < owners)
        def _():
            arrive(z + d, k)
            when(z > 0, lambda: send_on(z + d, k, 0))
            pass_piece(z + d, k, c).start()

    upper = z >= owners // 2
    near = jnp.where(upper, owners - 1 - z, z)

    def source(i):
        walk = jnp.where(i > near, i, near - i)
        return jnp.where(upper, owners - 1 - walk, walk)

    lane = lax.broadcasted_iota(jnp.int32, (rows, experts), 1)

    def expert(b, slot, e):
        both = dot(blocks[b], gate_up[e])
        column = jnp.transpose(scales[b])
        factor = jnp.sum(jnp.where(lane == z * local + e, column, 0.0), axis=1, keepdims=True)
        value = silu(both[:, 0:ff]) * both[:, ff:] * factor
        hidden[slot, :, pl.ds(pl.multiple_of(e * ff, LANES), ff)] = value.astype(bf16)

    def columns(core, p):
        return pl.ds(pl.multiple_of(core * half + parts[p][0], LANES), parts[p][1])

    def shared_first(j, block):
        both = dot(block, shared_in[...])
        shared_hidden[j] = (silu(both[:, 0:sff]) * both[:, sff:]).astype(bf16)

    early = max(local - 3, 0)

    def own(e, carry):
        expert_loads(e)[0].wait()
        expert_loads(e)[1].wait()
        expert(z, 0, e)
        when(e == early, lambda: fetch(1, 0))
        return carry

    lax.fori_loop(0, local, own, 0)
    for k in range(1, PIECES):
        fetch(1, k)

    def take_peer(k):
        here = peers.at[k - 1, pl.ds(pl.multiple_of(c * share, share), share)]
        pltpu.make_async_copy(here, here, grecv.at[k - 1]).wait()
        pass_peer(k, c).start()

    for k in range(1, min(groups, 3)):
        take_peer(k)
    shared_loads[0].wait()
    shared_loads[1].wait()
    shared_first(0, blocks[z])

    def shared_all():
        for k in range(3, groups):
            take_peer(k)
        for j in range(1, groups):
            pass_peer(j, other).wait_recv()
            shared_first(j, peers[j - 1])
        shared_loads[2].wait()
        for j in range(1, groups):
            at = pl.ds(pl.multiple_of(other * half, LANES), half)
            shared_staged[j - 1] = dot(shared_hidden[j], shared_out[:, at]).astype(bf16)
            shared_exchange(j).start()
        for j in range(1, groups):
            at = pl.ds(pl.multiple_of(c * half, LANES), half)
            keep[...] = dot(shared_hidden[j], shared_out[:, at])
            shared_exchange(j).wait()
            summed = keep[...] + partner_shared[j - 1].astype(f32)
            partner_shared[j - 1] = summed.astype(bf16)
            shared_result(j).start()

    def routed(i, carry):
        b = source(i)
        for k in range(PIECES):
            pass_piece(b, k, other).wait_recv()
        for e in range(local):
            expert(b, 1, e)
            if e == local // 2 - 1:
                when(i + 1 < owners, lambda: fetch(i + 1, 0))
        if local < 2:
            when(i + 1 < owners, lambda: fetch(i + 1, 0))

        @pl.when(i == 1)
        def _():
            for e in range(local):
                expert_loads(e)[2].wait()

        for p in range(2):
            at = pl.ds(*parts[p])
            staged[:, at] = dot(hidden[1], down[:, columns(other, p)]).astype(bf16)
            exchange(i, p).start()
        for k in range(1, PIECES):
            when(i + 1 < owners, lambda: fetch(i + 1, k))
        for p in range(2):
            keep[:, pl.ds(*parts[p])] = dot(hidden[1], down[:, columns(c, p)])
        slot = lax.rem(z - b + owners, owners) - 1
        for p in range(2):
            at = pl.ds(*parts[p])
            exchange(i, p).wait()
            summed = keep[:, at] + partner_routed[i, :, at].astype(f32)
            partner_routed[i, :, at] = summed.astype(bf16)
            result_send(i, p, slot, b).start()
        when(i == 1, shared_all)
        return carry

    lax.fori_loop(1, owners, routed, 0)

    for p in range(2):
        at = pl.ds(*parts[p])
        value = dot(hidden[0], down[:, columns(other, p)])
        value = value + dot(shared_hidden[0], shared_out[:, columns(other, p)])
        staged[:, at] = value.astype(bf16)
        exchange(0, p).start()
    for p in range(2):
        value = dot(hidden[0], down[:, columns(c, p)])
        total[:, pl.ds(*parts[p])] = value + dot(shared_hidden[0], shared_out[:, columns(c, p)])
    for p in range(2):
        at = pl.ds(*parts[p])
        exchange(0, p).wait()
        total[:, at] = total[:, at] + partner_routed[0, :, at].astype(f32)

    for j in range(1, groups):
        shared_result(j).wait_recv()
        total[...] = total[...] + landed[owners - 1 + j - 1].astype(f32)

    def gather(i, carry):
        slot = lax.rem(source(i) - z + owners, owners) - 1
        for p in range(2):
            result_send(0, p, slot, z).wait_recv()
        total[...] = total[...] + landed[slot].astype(f32)
        return carry

    lax.fori_loop(1, owners, gather, 0)
    staged[...] = total[...].astype(bf16)
    store = pltpu.make_async_copy(staged, out, token_sem.at[0])
    store.start()

    def drained(i, carry):
        b = source(i)
        slot = lax.rem(z - b + owners, owners) - 1
        for k in range(PIECES):
            pass_piece(b, k, c).wait_send()
        for p in range(2):
            result_send(i, p, slot, b).wait_send()
        return carry

    lax.fori_loop(1, owners, drained, 0)

    def sent(b, carry):
        @pl.when((b <= z) & (z + 1 < owners))
        def _():
            for k in range(PIECES):
                piece_send(b, k, 1).wait_send()
            scale_send(b, 1).wait_send()

        @pl.when((b >= z) & (z > 0))
        def _():
            for k in range(PIECES):
                piece_send(b, k, 0).wait_send()
            scale_send(b, 0).wait_send()

        return carry

    lax.fori_loop(0, owners, sent, 0)
    for k in range(1, groups):
        peer_send(k).wait_send()
        pass_peer(k, c).wait_send()
        shared_result(k).wait_send()
    store.wait()


def on_device(owners, groups, tokens, norm_gain, expert_ids, route_weights, *matrices):
    w_gate, w_up, w_down, shared_gate, shared_up, shared_down = matrices
    rows, width = tokens.shape
    half = width // 2
    local, ff, _ = w_down.shape
    sff = shared_down.shape[0]
    top = expert_ids.shape[1]
    bf16, f32 = jnp.bfloat16, jnp.float32
    dma = pltpu.SemaphoreType.DMA
    anywhere = pl.BlockSpec(memory_space=pl.ANY)
    return pl.pallas_call(
        functools.partial(kernel, owners, groups),
        out_shape=jax.ShapeDtypeStruct((rows, half), bf16),
        in_specs=[anywhere] * 10,
        out_specs=anywhere,
        scratch_shapes=[
            pltpu.VMEM((owners, rows, width), bf16),
            pltpu.VMEM((owners, local * owners, rows), f32),
            pltpu.VMEM((groups - 1, rows, width), bf16),
            pltpu.VMEM((local, width, 2 * ff), bf16),
            pltpu.VMEM((local * ff, width), bf16),
            pltpu.VMEM((width, 2 * sff), bf16),
            pltpu.VMEM((sff, width), bf16),
            pltpu.VMEM((2, rows, local * ff), bf16),
            pltpu.VMEM((groups, rows, sff), bf16),
            pltpu.VMEM((rows, half), bf16),
            pltpu.VMEM((groups - 1, rows, half), bf16),
            pltpu.VMEM((rows, half), f32),
            pltpu.VMEM((rows, half), f32),
            pltpu.VMEM((owners, rows, half), bf16),
            pltpu.VMEM((groups - 1, rows, half), bf16),
            pltpu.VMEM((owners + groups - 2, rows, half), bf16),
            pltpu.VMEM((1, width), f32),
            pltpu.VMEM((top, rows), jnp.int32),
            pltpu.VMEM((top, rows), jnp.int32),
            dma((3, local)),
            dma((3,)),
            dma((2,)),
            dma((3,)),
            dma((2, owners, PIECES)),
            dma((owners, PIECES)),
            dma((2, owners)),
            dma((owners,)),
            dma((groups - 1,)),
            dma((groups - 1,)),
            dma((owners, PIECES)),
            dma((owners, PIECES)),
            dma((groups - 1,)),
            dma((groups - 1,)),
            dma((owners, 2)),
            dma((owners, 2)),
            dma((groups - 1,)),
            dma((groups - 1,)),
            dma((owners - 1, 2)),
            dma((owners - 1, 2)),
            dma((groups - 1,)),
            dma((groups - 1,)),
        ],
        compiler_params=pltpu.CompilerParams(
            collective_id=0, has_side_effects=True, vmem_limit_bytes=VMEM_BYTES
        ),
    )(tokens, norm_gain[None, :], expert_ids.T, route_weights.T, *matrices)


def solution(mesh):
    placed = (
        P(("dp", "expert"), None),
        P(),
        P(("dp", "expert"), None),
        P(("dp", "expert"), None),
        P("expert", None, "tensor"),
        P("expert", None, "tensor"),
        P("expert", "tensor", None),
        P(None, ("dp", "tensor")),
        P(None, ("dp", "tensor")),
        P(("dp", "tensor"), None),
    )
    return jax.shard_map(
        functools.partial(on_device, mesh.shape["expert"], mesh.shape["dp"]),
        mesh=mesh,
        in_specs=placed,
        out_specs=P(("dp", "expert"), "tensor"),
        check_vma=False,
    )
```

```python
import functools

import jax
import jax.numpy as jnp
from jax import lax
from jax.experimental import pallas as pl
from jax.experimental.pallas import tpu as pltpu
from jax.sharding import PartitionSpec as P

EPSILON = 1e-06
LANES = 128
PIECES = 2
TILE = 256
MESH = pl.DeviceIdType.MESH
VMEM_BYTES = 66400000


def dot(a, b):
    return jnp.dot(a, b, preferred_element_type=jnp.float32)


def silu(v):
    return v / (1.0 + jnp.exp(-v))


def kernel(
    owners,
    groups,
    tokens,
    gain_in,
    ids_in,
    weights_in,
    w_gate,
    w_up,
    w_down,
    shared_gate,
    shared_up,
    shared_down,
    out,
    blocks,
    scales,
    peers,
    gate_up,
    down,
    shared_in,
    shared_out,
    hidden,
    shared_hidden,
    staged,
    shared_staged,
    keep,
    relay,
    partner_routed,
    partner_shared,
    landed,
    gain,
    ids,
    weights,
    load_sem,
    shared_sem,
    token_sem,
    small_sem,
    zsend,
    zrecv,
    ssend,
    srecv,
    gsend,
    grecv,
    fsend,
    frecv,
    psend,
    precv,
    esend,
    erecv,
    xsend,
    xrecv,
    rsend,
    rrecv,
    qsend,
    qrecv,
    msend,
    mrecv,
    nsend,
    nrecv,
):
    g = lax.axis_index("dp")
    z = lax.axis_index("expert")
    c = lax.axis_index("tensor")
    other = 1 - c
    local, ff, width = w_down.shape
    sff = shared_down.shape[0]
    rows = tokens.shape[0]
    half = width // 2
    experts = local * owners
    share = rows // 2
    piece = share // PIECES
    f32, bf16 = jnp.float32, jnp.bfloat16
    cut = -(-half // (2 * TILE)) * TILE
    parts = ((0, cut), (cut, half - cut))
    tiles = [
        [(at, min(TILE, first + size - at)) for at in range(first, first + size, TILE)]
        for first, size in parts
    ]
    merge = owners > 3
    at_end = (z == 0) | (z == owners - 1)
    by_end = (z == 1) | (z == owners - 2)
    last = owners - 1

    def rows_of(core, k):
        return pl.ds(pl.multiple_of(core * share + k * piece, piece), piece)

    token_loads = [
        pltpu.make_async_copy(
            tokens.at[pl.ds(pl.multiple_of(core * share, share), share)],
            blocks.at[z, pl.ds(pl.multiple_of(core * share, share), share)],
            token_sem.at[p],
        )
        for p, core in enumerate((c, other))
    ]
    small_loads = [
        pltpu.make_async_copy(gain_in, gain.at[0], small_sem.at[0]),
        pltpu.make_async_copy(ids_in, ids, small_sem.at[1]),
        pltpu.make_async_copy(weights_in, weights, small_sem.at[2]),
    ]
    barrier = pltpu.get_barrier_semaphore()
    for r in range(1, owners):
        peer = {"expert": lax.rem(z + r, owners)}
        pl.semaphore_signal(barrier, inc=1, device_id=peer, device_id_type=MESH)
    for r in range(1, groups):
        peer = {"dp": lax.rem(g + r, groups)}
        pl.semaphore_signal(barrier, inc=1, device_id=peer, device_id_type=MESH)
    pl.semaphore_signal(barrier, inc=1, device_id={"tensor": other}, device_id_type=MESH)
    for load in token_loads + small_loads:
        load.start()

    def expert_loads(e):
        first = pl.ds(pl.multiple_of(e * ff, LANES), ff)
        return (
            pltpu.make_async_copy(w_gate.at[e], gate_up.at[e, :, pl.ds(0, ff)], load_sem.at[0, e]),
            pltpu.make_async_copy(w_up.at[e], gate_up.at[e, :, pl.ds(ff, ff)], load_sem.at[1, e]),
            pltpu.make_async_copy(w_down.at[e], down.at[first], load_sem.at[2, e]),
        )

    shared_loads = (
        pltpu.make_async_copy(shared_gate, shared_in.at[:, pl.ds(0, sff)], shared_sem.at[0]),
        pltpu.make_async_copy(shared_up, shared_in.at[:, pl.ds(sff, sff)], shared_sem.at[1]),
        pltpu.make_async_copy(shared_down, shared_out, shared_sem.at[2]),
    )

    def load_first(e, carry):
        expert_loads(e)[0].start()
        expert_loads(e)[1].start()
        return carry

    def load_second(e, carry):
        expert_loads(e)[2].start()
        return carry

    lax.fori_loop(0, local - local // 4, load_first, 0)
    shared_loads[0].start()
    shared_loads[1].start()
    lax.fori_loop(local - local // 4, local, load_first, 0)
    lax.fori_loop(0, local, load_second, 0)
    shared_loads[2].start()

    for load in small_loads:
        load.wait()
    lane_expert = lax.broadcasted_iota(jnp.int32, (experts, rows), 0)
    scale = jnp.zeros((experts, rows), f32)
    for k in range(ids.shape[0]):
        weight = weights[k : k + 1, :].astype(f32) * (1.0 / 64.0)
        scale = scale + jnp.where(ids[k : k + 1, :] == lane_expert, weight, 0.0)
    scales[z] = scale

    step = 16

    def norm(core):
        def body(t, carry):
            span = pl.ds(pl.multiple_of(core * share + t * step, step), step)
            value = blocks[z, span, :].astype(f32)
            square = jnp.sum(value * value, axis=1, keepdims=True)
            inverse = lax.rsqrt(square / width + EPSILON)
            blocks[z, span, :] = (value * inverse * gain[...]).astype(bf16)
            return carry

        lax.fori_loop(0, share // step, body, 0)

    def piece_send(b, k, way):
        return pltpu.make_async_remote_copy(
            src_ref=blocks.at[b, rows_of(c, k)],
            dst_ref=blocks.at[b, rows_of(c, k)],
            send_sem=zsend.at[way, b, k],
            recv_sem=zrecv.at[b, k],
            device_id={"expert": lax.rem(z + (1 if way else owners - 1), owners)},
            device_id_type=MESH,
        )

    def scale_send(b, way):
        return pltpu.make_async_remote_copy(
            src_ref=scales.at[b],
            dst_ref=scales.at[b],
            send_sem=ssend.at[way, b],
            recv_sem=srecv.at[b],
            device_id={"expert": lax.rem(z + (1 if way else owners - 1), owners)},
            device_id_type=MESH,
        )

    pairs = groups // 2 if groups % 2 == 0 else groups
    lows = groups // pairs

    def mate(k, sign):
        high, low = k // lows, k % lows
        up = lax.rem(g // lows + (high if sign > 0 else pairs - high), pairs)
        return up * lows + lax.rem(lax.rem(g, lows) + (low if sign > 0 else lows - low), lows)

    def peer_rows(k, core):
        return pl.ds(pl.multiple_of((k - 1) * rows + core * share, share), share)

    def peer_send(k):
        mine = pl.ds(pl.multiple_of(c * share, share), share)
        return pltpu.make_async_remote_copy(
            src_ref=blocks.at[z, mine],
            dst_ref=peers.at[peer_rows(k, c)],
            send_sem=gsend.at[k - 1],
            recv_sem=grecv.at[k - 1],
            device_id={"dp": mate(k, 1)},
            device_id_type=MESH,
        )

    def pass_piece(b, k, core):
        return pltpu.make_async_remote_copy(
            src_ref=blocks.at[b, rows_of(core, k)],
            dst_ref=blocks.at[b, rows_of(core, k)],
            send_sem=fsend.at[b, k],
            recv_sem=frecv.at[b, k],
            device_id={"tensor": other},
            device_id_type=MESH,
        )

    def pass_peer(k, core):
        return pltpu.make_async_remote_copy(
            src_ref=peers.at[peer_rows(k, core)],
            dst_ref=peers.at[peer_rows(k, core)],
            send_sem=psend.at[k - 1],
            recv_sem=precv.at[k - 1],
            device_id={"tensor": other},
            device_id_type=MESH,
        )

    def exchange(i, p):
        at = pl.ds(*parts[p])
        return pltpu.make_async_remote_copy(
            src_ref=staged.at[:, at],
            dst_ref=partner_routed.at[i, :, at],
            send_sem=esend.at[i, p],
            recv_sem=erecv.at[i, p],
            device_id={"tensor": other},
            device_id_type=MESH,
        )

    def result_send(i, p, slot, b):
        at = pl.ds(*parts[p])
        return pltpu.make_async_remote_copy(
            src_ref=partner_routed.at[i, :, at],
            dst_ref=landed.at[slot, :, at],
            send_sem=rsend.at[slot, p],
            recv_sem=rrecv.at[slot, p],
            device_id={"expert": b},
            device_id_type=MESH,
        )

    def relay_send(at):
        return pltpu.make_async_remote_copy(
            src_ref=partner_routed.at[last, :, pl.ds(*at)],
            dst_ref=relay.at[:, pl.ds(*at)],
            send_sem=nsend.at[at[0] // TILE],
            recv_sem=nrecv.at[at[0] // TILE],
            device_id={"expert": jnp.where(z == 0, 1, owners - 2)},
            device_id_type=MESH,
        )

    def merged_send(at):
        return pltpu.make_async_remote_copy(
            src_ref=partner_routed.at[last, :, pl.ds(*at)],
            dst_ref=landed.at[jnp.where(z == 1, 1, owners - 3), :, pl.ds(*at)],
            send_sem=msend.at[at[0] // TILE],
            recv_sem=mrecv.at[at[0] // TILE],
            device_id={"expert": jnp.where(z == 1, owners - 1, 0)},
            device_id_type=MESH,
        )

    def shared_exchange(j):
        return pltpu.make_async_remote_copy(
            src_ref=shared_staged.at[j - 1],
            dst_ref=partner_shared.at[j - 1],
            send_sem=xsend.at[j - 1],
            recv_sem=xrecv.at[j - 1],
            device_id={"tensor": other},
            device_id_type=MESH,
        )

    def shared_result(j):
        return pltpu.make_async_remote_copy(
            src_ref=partner_shared.at[j - 1],
            dst_ref=landed.at[owners - 1 + j - 1],
            send_sem=qsend.at[j - 1],
            recv_sem=qrecv.at[j - 1],
            device_id={"dp": mate(j, -1)},
            device_id_type=MESH,
        )

    token_loads[0].wait()
    norm(c)
    pl.semaphore_wait(barrier, owners + groups - 1)

    def when(condition, action):
        @pl.when(condition)
        def _():
            action()

    def send_on(b, k, way):
        piece_send(b, k, way).start()
        if k == 0:
            scale_send(b, way).start()

    for k in range(PIECES):
        when(z + 1 < owners, lambda: send_on(z, k, 1))
        when(z > 0, lambda: send_on(z, k, 0))
    for k in range(1, groups):
        peer_send(k).start()

    token_loads[1].wait()
    norm(other)

    def arrive(b, k):
        here = blocks.at[b, rows_of(c, k)]
        pltpu.make_async_copy(here, here, zrecv.at[b, k]).wait()
        if k == 0:
            pltpu.make_async_copy(scales.at[b], scales.at[b], srecv.at[b]).wait()

    def fetch(d, k):
        @pl.when(z - d >= 0)
        def _():
            arrive(z - d, k)
            when(z + 1 < owners, lambda: send_on(z - d, k, 1))
            pass_piece(z - d, k, c).start()

        @pl.when(z + d < owners)
        def _():
            arrive(z + d, k)
            when(z > 0, lambda: send_on(z + d, k, 0))
            pass_piece(z + d, k, c).start()

    upper = z >= owners // 2
    near = jnp.where(upper, owners - 1 - z, z)

    def source(i):
        step_out = jnp.where(lax.rem(i, 2) == 1, near + lax.div(i + 1, 2), near - lax.div(i, 2))
        walk = jnp.where(i > 2 * near, i, step_out)
        return jnp.where(upper, owners - 1 - walk, walk)

    lane = lax.broadcasted_iota(jnp.int32, (rows, experts), 1)

    def expert(b, slot, e):
        both = dot(blocks[b], gate_up[e])
        column = jnp.transpose(scales[b])
        factor = jnp.sum(jnp.where(lane == z * local + e, column, 0.0), axis=1, keepdims=True)
        value = silu(both[:, 0:ff]) * both[:, ff:] * factor
        hidden[slot, :, pl.ds(pl.multiple_of(e * ff, LANES), ff)] = value.astype(bf16)

    def columns(core, p):
        return pl.ds(pl.multiple_of(core * half + parts[p][0], LANES), parts[p][1])

    own_shared = pl.ds((groups - 1) * rows, rows)

    def shared_first(span, block):
        both = dot(block, shared_in[...])
        shared_hidden[span] = (silu(both[:, 0:sff]) * both[:, sff:]).astype(bf16)

    early = max(local - 3, 0)

    def own(e, carry):
        expert_loads(e)[0].wait()
        expert_loads(e)[1].wait()
        expert(z, 0, e)
        when(e == early, lambda: fetch(1, 0))
        return carry

    lax.fori_loop(0, local, own, 0)
    shared_loads[0].wait()
    shared_loads[1].wait()
    shared_first(own_shared, blocks[z])
    for k in range(1, PIECES):
        fetch(1, k)

    def take_peer(k):
        here = peers.at[peer_rows(k, c)]
        pltpu.make_async_copy(here, here, grecv.at[k - 1]).wait()
        pass_peer(k, c).start()

    for k in range(1, min(groups, 3)):
        take_peer(k)

    def shared_all():
        for k in range(3, groups):
            take_peer(k)
        for j in range(1, groups):
            pass_peer(j, other).wait_recv()
            span = pl.ds((j - 1) * rows, rows)
            shared_first(span, peers[span])
        shared_loads[2].wait()
        at = pl.ds(pl.multiple_of(other * half, LANES), half)
        for j in range(1, groups):
            span = pl.ds((j - 1) * rows, rows)
            shared_staged[j - 1] = dot(shared_hidden[span], shared_out[:, at]).astype(bf16)
            shared_exchange(j).start()

    def shared_rest():
        at = pl.ds(pl.multiple_of(c * half, LANES), half)
        for j in range(1, groups):
            shared_exchange(j).wait()
            value = dot(shared_hidden[pl.ds((j - 1) * rows, rows)], shared_out[:, at])
            partner_shared[j - 1] = (value + partner_shared[j - 1].astype(f32)).astype(bf16)
            shared_result(j).start()

    def direct(i):
        return (i < last) | jnp.logical_not(at_end | by_end) if merge else i > 0

    def send_result(i, p, slot, b):
        when(direct(i), lambda: result_send(i, p, slot, b).start())
        if merge:

            @pl.when((i == last) & at_end)
            def _():
                for at in tiles[p]:
                    relay_send(at).start()

    def routed(i, carry):
        b = source(i)
        for k in range(PIECES):
            pass_piece(b, k, other).wait_recv()
        for e in range(local):
            expert(b, 1, e)
            if e == local // 2 - 1:
                when(i + 1 < owners, lambda: fetch(i + 1, 0))
        if local < 2:
            when(i + 1 < owners, lambda: fetch(i + 1, 0))

        if owners > 2:
            when(i == 2, shared_rest)

        @pl.when(i == 1)
        def _():
            for e in range(local):
                expert_loads(e)[2].wait()

        for p in range(2):
            at = pl.ds(*parts[p])
            staged[:, at] = dot(hidden[1], down[:, columns(other, p)]).astype(bf16)
            exchange(i, p).start()
        for k in range(1, PIECES):
            when(i + 1 < owners, lambda: fetch(i + 1, k))
        for p in range(2):
            keep[:, pl.ds(*parts[p])] = dot(hidden[1], down[:, columns(c, p)])
        slot = lax.rem(z - b + owners, owners) - 1
        for p in range(2):
            at = pl.ds(*parts[p])
            exchange(i, p).wait()
            summed = keep[:, at] + partner_routed[i, :, at].astype(f32)
            partner_routed[i, :, at] = summed.astype(bf16)
            send_result(i, p, slot, b)
        when(i == 1, shared_all)
        if owners == 2:
            shared_rest()
        return carry

    lax.fori_loop(1, owners, routed, 0)

    for p in range(2):
        at = pl.ds(*parts[p])
        value = dot(hidden[0], down[:, columns(other, p)])
        value = value + dot(shared_hidden[own_shared], shared_out[:, columns(other, p)])
        staged[:, at] = value.astype(bf16)
        exchange(0, p).start()
    for p in range(2):
        value = dot(hidden[0], down[:, columns(c, p)])
        keep[:, pl.ds(*parts[p])] = value + dot(shared_hidden[own_shared], shared_out[:, columns(c, p)])
    for p in range(2):
        at = pl.ds(*parts[p])
        exchange(0, p).wait()
        keep[:, at] = keep[:, at] + partner_routed[0, :, at].astype(f32)

    every = tiles[0] + tiles[1]
    if merge:

        @pl.when(by_end)
        def _():
            for at in every:
                span = pl.ds(*at)
                pltpu.make_async_copy(relay.at[:, span], relay.at[:, span], nrecv.at[at[0] // TILE]).wait()
                value = partner_routed[last, :, span].astype(f32) + relay[:, span].astype(f32)
                partner_routed[last, :, span] = value.astype(bf16)
                merged_send(at).start()

    for j in range(1, groups):
        shared_result(j).wait_recv()
        keep[...] = keep[...] + landed[owners - 1 + j - 1].astype(f32)

    def gather(i, carry):
        slot = lax.rem(source(i) - z + owners, owners) - 1

        def arrived():
            for p in range(2):
                result_send(0, p, slot, z).wait_recv()
            keep[...] = keep[...] + landed[slot].astype(f32)

        when((i < last - 1) | jnp.logical_not(at_end) if merge else i > 0, arrived)
        return carry

    lax.fori_loop(1, owners, gather, 0)
    if merge:

        @pl.when(at_end)
        def _():
            slot = jnp.where(z == 0, owners - 3, 1)
            for at in every:
                span = pl.ds(*at)
                here = landed.at[slot, :, span]
                pltpu.make_async_copy(here, here, mrecv.at[at[0] // TILE]).wait()
                keep[:, span] = keep[:, span] + landed[slot, :, span].astype(f32)

    out[...] = keep[...].astype(bf16)

    def drained(i, carry):
        b = source(i)
        slot = lax.rem(z - b + owners, owners) - 1
        for k in range(PIECES):
            pass_piece(b, k, c).wait_send()

        def done():
            for p in range(2):
                result_send(i, p, slot, b).wait_send()

        when(direct(i), done)
        return carry

    lax.fori_loop(1, owners, drained, 0)

    if merge:

        @pl.when(at_end)
        def _():
            for at in every:
                relay_send(at).wait_send()

        @pl.when(by_end)
        def _():
            for at in every:
                merged_send(at).wait_send()

    def sent(b, carry):
        @pl.when((b <= z) & (z + 1 < owners))
        def _():
            for k in range(PIECES):
                piece_send(b, k, 1).wait_send()
            scale_send(b, 1).wait_send()

        @pl.when((b >= z) & (z > 0))
        def _():
            for k in range(PIECES):
                piece_send(b, k, 0).wait_send()
            scale_send(b, 0).wait_send()

        return carry

    lax.fori_loop(0, owners, sent, 0)
    for k in range(1, groups):
        peer_send(k).wait_send()
        pass_peer(k, c).wait_send()
        shared_result(k).wait_send()


def on_device(owners, groups, tokens, norm_gain, expert_ids, route_weights, *matrices):
    w_gate, w_up, w_down, shared_gate, shared_up, shared_down = matrices
    rows, width = tokens.shape
    half = width // 2
    local, ff, _ = w_down.shape
    sff = shared_down.shape[0]
    top = expert_ids.shape[1]
    tiles = -(-half // TILE)
    bf16, f32 = jnp.bfloat16, jnp.float32
    dma = pltpu.SemaphoreType.DMA
    anywhere = pl.BlockSpec(memory_space=pl.ANY)
    return pl.pallas_call(
        functools.partial(kernel, owners, groups),
        out_shape=jax.ShapeDtypeStruct((rows, half), bf16),
        in_specs=[anywhere] * 10,
        out_specs=pl.BlockSpec(memory_space=pltpu.VMEM),
        scratch_shapes=[
            pltpu.VMEM((owners, rows, width), bf16),
            pltpu.VMEM((owners, local * owners, rows), f32),
            pltpu.VMEM(((groups - 1) * rows, width), bf16),
            pltpu.VMEM((local, width, 2 * ff), bf16),
            pltpu.VMEM((local * ff, width), bf16),
            pltpu.VMEM((width, 2 * sff), bf16),
            pltpu.VMEM((sff, width), bf16),
            pltpu.VMEM((2, rows, local * ff), bf16),
            pltpu.VMEM((groups * rows, sff), bf16),
            pltpu.VMEM((rows, half), bf16),
            pltpu.VMEM((groups - 1, rows, half), bf16),
            pltpu.VMEM((rows, half), f32),
            pltpu.VMEM((rows, half), bf16),
            pltpu.VMEM((owners, rows, half), bf16),
            pltpu.VMEM((groups - 1, rows, half), bf16),
            pltpu.VMEM((owners + groups - 2, rows, half), bf16),
            pltpu.VMEM((1, width), f32),
            pltpu.VMEM((top, rows), jnp.int32),
            pltpu.VMEM((top, rows), jnp.int32),
            dma((3, local)),
            dma((3,)),
            dma((2,)),
            dma((3,)),
            dma((2, owners, PIECES)),
            dma((owners, PIECES)),
            dma((2, owners)),
            dma((owners,)),
            dma((groups - 1,)),
            dma((groups - 1,)),
            dma((owners, PIECES)),
            dma((owners, PIECES)),
            dma((groups - 1,)),
            dma((groups - 1,)),
            dma((owners, 2)),
            dma((owners, 2)),
            dma((groups - 1,)),
            dma((groups - 1,)),
            dma((owners - 1, 2)),
            dma((owners - 1, 2)),
            dma((groups - 1,)),
            dma((groups - 1,)),
            dma((tiles,)),
            dma((tiles,)),
            dma((tiles,)),
            dma((tiles,)),
        ],
        compiler_params=pltpu.CompilerParams(
            collective_id=0, has_side_effects=True, vmem_limit_bytes=VMEM_BYTES
        ),
    )(tokens, norm_gain, expert_ids.T, route_weights.T, *matrices)


def solution(mesh):
    placed = (
        P(("dp", "expert"), None),
        P(),
        P(("dp", "expert"), None),
        P(("dp", "expert"), None),
        P("expert", None, "tensor"),
        P("expert", None, "tensor"),
        P("expert", "tensor", None),
        P(None, ("dp", "tensor")),
        P(None, ("dp", "tensor")),
        P(("dp", "tensor"), None),
    )
    return jax.shard_map(
        functools.partial(on_device, mesh.shape["expert"], mesh.shape["dp"]),
        mesh=mesh,
        in_specs=placed,
        out_specs=P(("dp", "expert"), "tensor"),
        check_vma=False,
    )
```

```python
import functools

import jax
import jax.numpy as jnp
from jax import lax
from jax.experimental import pallas as pl
from jax.experimental.pallas import tpu as pltpu
from jax.sharding import PartitionSpec as P

EPSILON = 1e-06
LANES = 128
PIECES = 2
TILE = 256
MESH = pl.DeviceIdType.MESH
VMEM_BYTES = 66400000


def dot(a, b):
    return jnp.dot(a, b, preferred_element_type=jnp.float32)


def silu(v):
    return v / (1.0 + jnp.exp(-v))


def kernel(
    owners,
    groups,
    tokens,
    gain_in,
    ids_in,
    weights_in,
    w_gate,
    w_up,
    w_down,
    shared_gate,
    shared_up,
    shared_down,
    out,
    blocks,
    scales,
    peers,
    gate_up,
    down,
    shared_in,
    shared_out,
    hidden,
    shared_hidden,
    staged,
    shared_staged,
    keep,
    relay,
    partner_routed,
    partner_shared,
    landed,
    gain,
    ids,
    weights,
    load_sem,
    shared_sem,
    token_sem,
    small_sem,
    zsend,
    zrecv,
    ssend,
    srecv,
    gsend,
    grecv,
    fsend,
    frecv,
    psend,
    precv,
    esend,
    erecv,
    xsend,
    xrecv,
    rsend,
    rrecv,
    qsend,
    qrecv,
    msend,
    mrecv,
    nsend,
    nrecv,
):
    g = lax.axis_index("dp")
    z = lax.axis_index("expert")
    c = lax.axis_index("tensor")
    other = 1 - c
    local, ff, width = w_down.shape
    sff = shared_down.shape[0]
    rows = tokens.shape[0]
    half = width // 2
    experts = local * owners
    share = rows // 2
    piece = share // PIECES
    f32, bf16 = jnp.float32, jnp.bfloat16
    cut = -(-half // (2 * TILE)) * TILE
    parts = ((0, cut), (cut, half - cut))
    tiles = [
        [(at, min(TILE, first + size - at)) for at in range(first, first + size, TILE)]
        for first, size in parts
    ]
    merge = owners > 3
    at_end = (z == 0) | (z == owners - 1)
    by_end = (z == 1) | (z == owners - 2)
    last = owners - 1

    def rows_of(core, k):
        return pl.ds(pl.multiple_of(core * share + k * piece, piece), piece)

    token_loads = [
        pltpu.make_async_copy(
            tokens.at[pl.ds(pl.multiple_of(core * share, share), share)],
            blocks.at[z, pl.ds(pl.multiple_of(core * share, share), share)],
            token_sem.at[p],
        )
        for p, core in enumerate((c, other))
    ]
    small_loads = [
        pltpu.make_async_copy(gain_in, gain.at[0], small_sem.at[0]),
        pltpu.make_async_copy(ids_in, ids, small_sem.at[1]),
        pltpu.make_async_copy(weights_in, weights, small_sem.at[2]),
    ]
    barrier = pltpu.get_barrier_semaphore()
    for way in (1, owners - 1):

        @pl.when((z + 1 < owners) if way == 1 else (z > 0))
        def _():
            peer = {"expert": lax.rem(z + way, owners)}
            pl.semaphore_signal(barrier, inc=1, device_id=peer, device_id_type=MESH)

    for r in range(1, groups):
        peer = {"dp": lax.rem(g + r, groups)}
        pl.semaphore_signal(barrier, inc=1, device_id=peer, device_id_type=MESH)
    pl.semaphore_signal(barrier, inc=1, device_id={"tensor": other}, device_id_type=MESH)
    for load in token_loads + small_loads:
        load.start()

    def expert_loads(e):
        first = pl.ds(pl.multiple_of(e * ff, LANES), ff)
        return (
            pltpu.make_async_copy(w_gate.at[e], gate_up.at[e, :, pl.ds(0, ff)], load_sem.at[0, e]),
            pltpu.make_async_copy(w_up.at[e], gate_up.at[e, :, pl.ds(ff, ff)], load_sem.at[1, e]),
            pltpu.make_async_copy(w_down.at[e], down.at[first], load_sem.at[2, e]),
        )

    shared_loads = (
        pltpu.make_async_copy(shared_gate, shared_in.at[:, pl.ds(0, sff)], shared_sem.at[0]),
        pltpu.make_async_copy(shared_up, shared_in.at[:, pl.ds(sff, sff)], shared_sem.at[1]),
        pltpu.make_async_copy(shared_down, shared_out, shared_sem.at[2]),
    )

    def load_first(e, carry):
        expert_loads(e)[0].start()
        expert_loads(e)[1].start()
        return carry

    def load_second(e, carry):
        expert_loads(e)[2].start()
        return carry

    lax.fori_loop(0, local - local // 4, load_first, 0)
    shared_loads[0].start()
    shared_loads[1].start()
    lax.fori_loop(local - local // 4, local, load_first, 0)
    lax.fori_loop(0, local, load_second, 0)
    shared_loads[2].start()

    for load in small_loads:
        load.wait()
    lane_expert = lax.broadcasted_iota(jnp.int32, (experts, rows), 0)
    scale = jnp.zeros((experts, rows), f32)
    for k in range(ids.shape[0]):
        weight = weights[k : k + 1, :].astype(f32) * (1.0 / 64.0)
        scale = scale + jnp.where(ids[k : k + 1, :] == lane_expert, weight, 0.0)
    scales[z] = scale

    step = 16

    def norm(core):
        def body(t, carry):
            span = pl.ds(pl.multiple_of(core * share + t * step, step), step)
            value = blocks[z, span, :].astype(f32)
            square = jnp.sum(value * value, axis=1, keepdims=True)
            inverse = lax.rsqrt(square / width + EPSILON)
            blocks[z, span, :] = (value * inverse * gain[...]).astype(bf16)
            return carry

        lax.fori_loop(0, share // step, body, 0)

    def piece_send(b, k, way):
        return pltpu.make_async_remote_copy(
            src_ref=blocks.at[b, rows_of(c, k)],
            dst_ref=blocks.at[b, rows_of(c, k)],
            send_sem=zsend.at[way, b, k],
            recv_sem=zrecv.at[b, k],
            device_id={"expert": lax.rem(z + (1 if way else owners - 1), owners)},
            device_id_type=MESH,
        )

    def scale_send(b, way):
        return pltpu.make_async_remote_copy(
            src_ref=scales.at[b],
            dst_ref=scales.at[b],
            send_sem=ssend.at[way, b],
            recv_sem=srecv.at[b],
            device_id={"expert": lax.rem(z + (1 if way else owners - 1), owners)},
            device_id_type=MESH,
        )

    pairs = groups // 2 if groups % 2 == 0 else groups
    lows = groups // pairs

    def mate(k, sign):
        high, low = k // lows, k % lows
        up = lax.rem(g // lows + (high if sign > 0 else pairs - high), pairs)
        return up * lows + lax.rem(lax.rem(g, lows) + (low if sign > 0 else lows - low), lows)

    def peer_rows(k, core):
        return pl.ds(pl.multiple_of((k - 1) * rows + core * share, share), share)

    def peer_send(k):
        mine = pl.ds(pl.multiple_of(c * share, share), share)
        return pltpu.make_async_remote_copy(
            src_ref=blocks.at[z, mine],
            dst_ref=peers.at[peer_rows(k, c)],
            send_sem=gsend.at[k - 1],
            recv_sem=grecv.at[k - 1],
            device_id={"dp": mate(k, 1)},
            device_id_type=MESH,
        )

    def pass_piece(b, k, core):
        return pltpu.make_async_remote_copy(
            src_ref=blocks.at[b, rows_of(core, k)],
            dst_ref=blocks.at[b, rows_of(core, k)],
            send_sem=fsend.at[b, k],
            recv_sem=frecv.at[b, k],
            device_id={"tensor": other},
            device_id_type=MESH,
        )

    def pass_peer(k, core):
        return pltpu.make_async_remote_copy(
            src_ref=peers.at[peer_rows(k, core)],
            dst_ref=peers.at[peer_rows(k, core)],
            send_sem=psend.at[k - 1],
            recv_sem=precv.at[k - 1],
            device_id={"tensor": other},
            device_id_type=MESH,
        )

    def exchange(i, p):
        at = pl.ds(*parts[p])
        return pltpu.make_async_remote_copy(
            src_ref=staged.at[:, at],
            dst_ref=partner_routed.at[i, :, at],
            send_sem=esend.at[i, p],
            recv_sem=erecv.at[i, p],
            device_id={"tensor": other},
            device_id_type=MESH,
        )

    def result_send(i, p, slot, b):
        at = pl.ds(*parts[p])
        return pltpu.make_async_remote_copy(
            src_ref=partner_routed.at[i, :, at],
            dst_ref=landed.at[slot, :, at],
            send_sem=rsend.at[slot, p],
            recv_sem=rrecv.at[slot, p],
            device_id={"expert": b},
            device_id_type=MESH,
        )

    def relay_send(at):
        return pltpu.make_async_remote_copy(
            src_ref=partner_routed.at[last, :, pl.ds(*at)],
            dst_ref=relay.at[:, pl.ds(*at)],
            send_sem=nsend.at[at[0] // TILE],
            recv_sem=nrecv.at[at[0] // TILE],
            device_id={"expert": jnp.where(z == 0, 1, owners - 2)},
            device_id_type=MESH,
        )

    def merged_send(at):
        return pltpu.make_async_remote_copy(
            src_ref=partner_routed.at[last, :, pl.ds(*at)],
            dst_ref=landed.at[jnp.where(z == 1, 1, owners - 3), :, pl.ds(*at)],
            send_sem=msend.at[at[0] // TILE],
            recv_sem=mrecv.at[at[0] // TILE],
            device_id={"expert": jnp.where(z == 1, owners - 1, 0)},
            device_id_type=MESH,
        )

    def shared_exchange(j):
        return pltpu.make_async_remote_copy(
            src_ref=shared_staged.at[j - 1],
            dst_ref=partner_shared.at[j - 1],
            send_sem=xsend.at[j - 1],
            recv_sem=xrecv.at[j - 1],
            device_id={"tensor": other},
            device_id_type=MESH,
        )

    def shared_result(j):
        return pltpu.make_async_remote_copy(
            src_ref=partner_shared.at[j - 1],
            dst_ref=landed.at[owners - 1 + j - 1],
            send_sem=qsend.at[j - 1],
            recv_sem=qrecv.at[j - 1],
            device_id={"dp": mate(j, -1)},
            device_id_type=MESH,
        )

    token_loads[0].wait()
    norm(c)
    pl.semaphore_wait(barrier, groups + 2 - at_end.astype(jnp.int32))

    def when(condition, action):
        @pl.when(condition)
        def _():
            action()

    def send_on(b, k, way):
        piece_send(b, k, way).start()
        if k == 0:
            scale_send(b, way).start()

    for k in range(PIECES):
        when(z + 1 < owners, lambda: send_on(z, k, 1))
        when(z > 0, lambda: send_on(z, k, 0))
    for k in range(1, groups):
        peer_send(k).start()

    token_loads[1].wait()
    norm(other)

    def arrive(b, k):
        here = blocks.at[b, rows_of(c, k)]
        pltpu.make_async_copy(here, here, zrecv.at[b, k]).wait()
        if k == 0:
            pltpu.make_async_copy(scales.at[b], scales.at[b], srecv.at[b]).wait()

    def fetch(d, k):
        @pl.when(z - d >= 0)
        def _():
            arrive(z - d, k)
            when(z + 1 < owners, lambda: send_on(z - d, k, 1))
            pass_piece(z - d, k, c).start()

        @pl.when(z + d < owners)
        def _():
            arrive(z + d, k)
            when(z > 0, lambda: send_on(z + d, k, 0))
            pass_piece(z + d, k, c).start()

    upper = z >= owners // 2
    near = jnp.where(upper, owners - 1 - z, z)

    def source(i):
        step_out = jnp.where(lax.rem(i, 2) == 1, near + lax.div(i + 1, 2), near - lax.div(i, 2))
        walk = jnp.where(i > 2 * near, i, step_out)
        return jnp.where(upper, owners - 1 - walk, walk)

    lane = lax.broadcasted_iota(jnp.int32, (rows, experts), 1)

    def expert(b, slot, e):
        both = dot(blocks[b], gate_up[e])
        column = jnp.transpose(scales[b])
        factor = jnp.sum(jnp.where(lane == z * local + e, column, 0.0), axis=1, keepdims=True)
        value = silu(both[:, 0:ff]) * both[:, ff:] * factor
        hidden[slot, :, pl.ds(pl.multiple_of(e * ff, LANES), ff)] = value.astype(bf16)

    def columns(core, p):
        return pl.ds(pl.multiple_of(core * half + parts[p][0], LANES), parts[p][1])

    own_shared = pl.ds((groups - 1) * rows, rows)

    def shared_first(span, block):
        both = dot(block, shared_in[...])
        shared_hidden[span] = (silu(both[:, 0:sff]) * both[:, sff:]).astype(bf16)

    early = max(local - 3, 0)
    hook = local * 3 // 4 - 1 if local > 1 else 0

    def own(e, carry):
        expert_loads(e)[0].wait()
        expert_loads(e)[1].wait()
        expert(z, 0, e)
        when(e == early, lambda: fetch(1, 0))
        return carry

    lax.fori_loop(0, local, own, 0)
    shared_loads[0].wait()
    shared_loads[1].wait()
    shared_first(own_shared, blocks[z])
    for k in range(1, PIECES):
        fetch(1, k)

    def take_peer(k):
        here = peers.at[peer_rows(k, c)]
        pltpu.make_async_copy(here, here, grecv.at[k - 1]).wait()
        pass_peer(k, c).start()

    split = min(groups, 3)
    late, early_ones = range(1, split), range(split, groups)

    def take_peers(some):
        for k in some:
            take_peer(k)

    def shared_all(some):
        if not some:
            return
        if some is early_ones:
            shared_loads[2].wait()
            take_peers(late)
        for j in some:
            pass_peer(j, other).wait_recv()
        span = pl.ds((some[0] - 1) * rows, len(some) * rows)
        shared_first(span, peers[span])
        at = pl.ds(pl.multiple_of(other * half, LANES), half)
        value = dot(shared_hidden[span], shared_out[:, at])
        for n, j in enumerate(some):
            shared_staged[j - 1] = value[n * rows : (n + 1) * rows].astype(bf16)
            shared_exchange(j).start()

    def shared_rest(some):
        at = pl.ds(pl.multiple_of(c * half, LANES), half)
        for j in some:
            shared_exchange(j).wait()
            value = dot(shared_hidden[pl.ds((j - 1) * rows, rows)], shared_out[:, at])
            partner_shared[j - 1] = (value + partner_shared[j - 1].astype(f32)).astype(bf16)
            shared_result(j).start()

    def direct(i):
        return (i < last) | jnp.logical_not(at_end | by_end) if merge else i > 0

    def send_result(i, p, slot, b):
        when(direct(i), lambda: result_send(i, p, slot, b).start())
        if merge:

            @pl.when((i == last) & at_end)
            def _():
                for at in tiles[p]:
                    relay_send(at).start()

    def routed(i, carry):
        b = source(i)
        for k in range(PIECES):
            pass_piece(b, k, other).wait_recv()
        for e in range(local):
            expert(b, 1, e)
            if e == hook:
                when(i + 1 < owners, lambda: fetch(i + 1, 0))

        if owners > 2:
            when(i == 2, lambda: shared_rest(early_ones))

        @pl.when(i == 1)
        def _():
            for e in range(local):
                expert_loads(e)[2].wait()

        for p in range(2):
            at = pl.ds(*parts[p])
            staged[:, at] = dot(hidden[1], down[:, columns(other, p)]).astype(bf16)
            exchange(i, p).start()
        for k in range(1, PIECES):
            when(i + 1 < owners, lambda: fetch(i + 1, k))
        when(i == 1, lambda: take_peers(early_ones))
        for p in range(2):
            keep[:, pl.ds(*parts[p])] = dot(hidden[1], down[:, columns(c, p)])
        slot = lax.rem(z - b + owners, owners) - 1
        for p in range(2):
            at = pl.ds(*parts[p])
            exchange(i, p).wait()
            summed = keep[:, at] + partner_routed[i, :, at].astype(f32)
            partner_routed[i, :, at] = summed.astype(bf16)
            send_result(i, p, slot, b)
        when(i == 1, lambda: shared_all(early_ones))
        if owners == 2:
            shared_rest(early_ones)
        return carry

    lax.fori_loop(1, owners, routed, 0)

    shared_all(late)
    for p in range(2):
        at = pl.ds(*parts[p])
        value = dot(hidden[0], down[:, columns(other, p)])
        value = value + dot(shared_hidden[own_shared], shared_out[:, columns(other, p)])
        staged[:, at] = value.astype(bf16)
        exchange(0, p).start()
    shared_rest(late)

    every = tiles[0] + tiles[1]
    if merge:

        @pl.when(by_end)
        def _():
            for at in every:
                span = pl.ds(*at)
                pltpu.make_async_copy(relay.at[:, span], relay.at[:, span], nrecv.at[at[0] // TILE]).wait()
                value = partner_routed[last, :, span].astype(f32) + relay[:, span].astype(f32)
                partner_routed[last, :, span] = value.astype(bf16)
                merged_send(at).start()

    for p in range(2):
        value = dot(hidden[0], down[:, columns(c, p)])
        keep[:, pl.ds(*parts[p])] = value + dot(shared_hidden[own_shared], shared_out[:, columns(c, p)])
    for p in range(2):
        at = pl.ds(*parts[p])
        exchange(0, p).wait()
        keep[:, at] = keep[:, at] + partner_routed[0, :, at].astype(f32)

    def drained(i, carry):
        b = source(i)
        slot = lax.rem(z - b + owners, owners) - 1
        for k in range(PIECES):
            pass_piece(b, k, c).wait_send()

        def done():
            for p in range(2):
                result_send(i, p, slot, b).wait_send()

        when(direct(i), done)
        return carry

    lax.fori_loop(1, owners, drained, 0)

    if merge:

        @pl.when(at_end)
        def _():
            for at in every:
                relay_send(at).wait_send()

        @pl.when(by_end)
        def _():
            for at in every:
                merged_send(at).wait_send()

    def sent(b, carry):
        @pl.when((b <= z) & (z + 1 < owners))
        def _():
            for k in range(PIECES):
                piece_send(b, k, 1).wait_send()
            scale_send(b, 1).wait_send()

        @pl.when((b >= z) & (z > 0))
        def _():
            for k in range(PIECES):
                piece_send(b, k, 0).wait_send()
            scale_send(b, 0).wait_send()

        return carry

    lax.fori_loop(0, owners, sent, 0)
    for k in range(1, groups):
        peer_send(k).wait_send()
        pass_peer(k, c).wait_send()
        shared_result(k).wait_send()

    for j in range(1, groups):
        shared_result(j).wait_recv()
        keep[...] = keep[...] + landed[owners - 1 + j - 1].astype(f32)

    def gather(i, carry):
        slot = lax.rem(source(i) - z + owners, owners) - 1

        def arrived():
            for p in range(2):
                result_send(0, p, slot, z).wait_recv()
            keep[...] = keep[...] + landed[slot].astype(f32)

        when((i < last - 1) | jnp.logical_not(at_end) if merge else i > 0, arrived)
        return carry

    lax.fori_loop(1, owners, gather, 0)
    if merge:

        @pl.when(at_end)
        def _():
            slot = jnp.where(z == 0, owners - 3, 1)
            for at in every:
                span = pl.ds(*at)
                here = landed.at[slot, :, span]
                pltpu.make_async_copy(here, here, mrecv.at[at[0] // TILE]).wait()
                keep[:, span] = keep[:, span] + landed[slot, :, span].astype(f32)

    out[...] = keep[...].astype(bf16)


def on_device(owners, groups, tokens, norm_gain, expert_ids, route_weights, *matrices):
    w_gate, w_up, w_down, shared_gate, shared_up, shared_down = matrices
    rows, width = tokens.shape
    half = width // 2
    local, ff, _ = w_down.shape
    sff = shared_down.shape[0]
    top = expert_ids.shape[1]
    tiles = -(-half // TILE)
    bf16, f32 = jnp.bfloat16, jnp.float32
    dma = pltpu.SemaphoreType.DMA
    anywhere = pl.BlockSpec(memory_space=pl.ANY)
    result = pl.pallas_call(
        functools.partial(kernel, owners, groups),
        out_shape=pltpu.VMEM((rows, half), bf16),
        in_specs=[anywhere] * 10,
        out_specs=pl.BlockSpec(memory_space=pltpu.VMEM),
        scratch_shapes=[
            pltpu.VMEM((owners, rows, width), bf16),
            pltpu.VMEM((owners, local * owners, rows), f32),
            pltpu.VMEM(((groups - 1) * rows, width), bf16),
            pltpu.VMEM((local, width, 2 * ff), bf16),
            pltpu.VMEM((local * ff, width), bf16),
            pltpu.VMEM((width, 2 * sff), bf16),
            pltpu.VMEM((sff, width), bf16),
            pltpu.VMEM((2, rows, local * ff), bf16),
            pltpu.VMEM((groups * rows, sff), bf16),
            pltpu.VMEM((rows, half), bf16),
            pltpu.VMEM((groups - 1, rows, half), bf16),
            pltpu.VMEM((rows, half), f32),
            pltpu.VMEM((rows, half), bf16),
            pltpu.VMEM((owners, rows, half), bf16),
            pltpu.VMEM((groups - 1, rows, half), bf16),
            pltpu.VMEM((owners + groups - 2, rows, half), bf16),
            pltpu.VMEM((1, width), f32),
            pltpu.VMEM((top, rows), jnp.int32),
            pltpu.VMEM((top, rows), jnp.int32),
            dma((3, local)),
            dma((3,)),
            dma((2,)),
            dma((3,)),
            dma((2, owners, PIECES)),
            dma((owners, PIECES)),
            dma((2, owners)),
            dma((owners,)),
            dma((groups - 1,)),
            dma((groups - 1,)),
            dma((owners, PIECES)),
            dma((owners, PIECES)),
            dma((groups - 1,)),
            dma((groups - 1,)),
            dma((owners, 2)),
            dma((owners, 2)),
            dma((groups - 1,)),
            dma((groups - 1,)),
            dma((owners - 1, 2)),
            dma((owners - 1, 2)),
            dma((groups - 1,)),
            dma((groups - 1,)),
            dma((tiles,)),
            dma((tiles,)),
            dma((tiles,)),
            dma((tiles,)),
        ],
        compiler_params=pltpu.CompilerParams(
            collective_id=0, has_side_effects=True, vmem_limit_bytes=VMEM_BYTES
        ),
    )(tokens, norm_gain, expert_ids.T, route_weights.T, *matrices)
    return result


def solution(mesh):
    placed = (
        P(("dp", "expert"), None),
        P(),
        P(("dp", "expert"), None),
        P(("dp", "expert"), None),
        P("expert", None, "tensor"),
        P("expert", None, "tensor"),
        P("expert", "tensor", None),
        P(None, ("dp", "tensor")),
        P(None, ("dp", "tensor")),
        P(("dp", "tensor"), None),
    )
    return jax.shard_map(
        functools.partial(on_device, mesh.shape["expert"], mesh.shape["dp"]),
        mesh=mesh,
        in_specs=placed,
        out_specs=P(("dp", "expert"), "tensor"),
        check_vma=False,
    )
```

```python
import functools

import jax
import jax.numpy as jnp
from jax import lax
from jax.experimental import pallas as pl
from jax.experimental.pallas import tpu as pltpu
from jax.sharding import PartitionSpec as P

EPSILON = 1e-06
LANES = 128
PIECES = 2
TILE = 128
MESH = pl.DeviceIdType.MESH
VMEM_BYTES = 66400000


def dot(a, b):
    return jnp.dot(a, b, preferred_element_type=jnp.float32)


def silu(v):
    return v / (1.0 + jnp.exp(-v))


def kernel(
    owners,
    groups,
    tokens,
    gain_in,
    ids_in,
    weights_in,
    w_gate,
    w_up,
    w_down,
    shared_gate,
    shared_up,
    shared_down,
    out,
    blocks,
    scales,
    peers,
    gate_up,
    down,
    shared_in,
    shared_out,
    hidden,
    shared_hidden,
    staged,
    shared_staged,
    keep,
    relay,
    partner_routed,
    partner_shared,
    landed,
    gain,
    ids,
    weights,
    load_sem,
    down_sem,
    shared_sem,
    token_sem,
    small_sem,
    zsend,
    zrecv,
    ssend,
    srecv,
    gsend,
    grecv,
    fsend,
    frecv,
    psend,
    precv,
    esend,
    erecv,
    xsend,
    xrecv,
    rsend,
    rrecv,
    qsend,
    qrecv,
    msend,
    mrecv,
    nsend,
    nrecv,
):
    g = lax.axis_index("dp")
    z = lax.axis_index("expert")
    c = lax.axis_index("tensor")
    other = 1 - c
    local, ff, width = w_down.shape
    sff = shared_down.shape[0]
    rows = tokens.shape[0]
    half = width // 2
    experts = local * owners
    share = rows // 2
    piece = share // PIECES
    f32, bf16 = jnp.float32, jnp.bfloat16
    parts = ((0, half),)
    tiles = [
        [(at, min(TILE, first + size - at)) for at in range(first, first + size, TILE)]
        for first, size in parts
    ]
    merge = owners > 3
    at_end = (z == 0) | (z == owners - 1)
    by_end = (z == 1) | (z == owners - 2)
    last = owners - 1

    def rows_of(core, k):
        return pl.ds(pl.multiple_of(core * share + k * piece, piece), piece)

    token_loads = [
        pltpu.make_async_copy(
            tokens.at[pl.ds(pl.multiple_of(core * share, share), share)],
            blocks.at[z, pl.ds(pl.multiple_of(core * share, share), share)],
            token_sem.at[p],
        )
        for p, core in enumerate((c, other))
    ]
    small_loads = [
        pltpu.make_async_copy(gain_in, gain.at[0], small_sem.at[0]),
        pltpu.make_async_copy(ids_in, ids, small_sem.at[1]),
        pltpu.make_async_copy(weights_in, weights, small_sem.at[2]),
    ]
    barrier = pltpu.get_barrier_semaphore()
    for way in (1, owners - 1):

        @pl.when((z + 1 < owners) if way == 1 else (z > 0))
        def _():
            peer = {"expert": lax.rem(z + way, owners)}
            pl.semaphore_signal(barrier, inc=1, device_id=peer, device_id_type=MESH)

    for r in range(1, groups):
        peer = {"dp": lax.rem(g + r, groups)}
        pl.semaphore_signal(barrier, inc=1, device_id=peer, device_id_type=MESH)
    pl.semaphore_signal(barrier, inc=1, device_id={"tensor": other}, device_id_type=MESH)
    for load in token_loads + small_loads:
        load.start()

    def half_of(core):
        return pl.ds(pl.multiple_of(core * half, LANES), half)

    def settle(ref, sem):
        pltpu.make_async_copy(ref, ref, sem).wait()

    shared_loads = (
        pltpu.make_async_copy(shared_gate, shared_in.at[:, pl.ds(0, sff)], shared_sem.at[0]),
        pltpu.make_async_copy(shared_up, shared_in.at[:, pl.ds(sff, sff)], shared_sem.at[0]),
        pltpu.make_async_copy(shared_down.at[:, half_of(other)], shared_out.at[0], shared_sem.at[1]),
        pltpu.make_async_copy(shared_down.at[:, half_of(c)], shared_out.at[1], shared_sem.at[1]),
    )

    def load_first(e, carry):
        pltpu.make_async_copy(w_gate.at[e], gate_up.at[e, :, pl.ds(0, ff)], load_sem.at[e]).start()
        pltpu.make_async_copy(w_up.at[e], gate_up.at[e, :, pl.ds(ff, ff)], load_sem.at[e]).start()
        return carry

    def load_second(e, carry):
        first = pl.ds(pl.multiple_of(e * ff, LANES), ff)
        for n, core in enumerate((other, c)):
            part = w_down.at[e, :, half_of(core)]
            pltpu.make_async_copy(part, down.at[n, first], down_sem.at[n]).start()
        return carry

    lax.fori_loop(0, local - local // 4, load_first, 0)
    shared_loads[0].start()
    shared_loads[1].start()
    lax.fori_loop(local - local // 4, local, load_first, 0)
    lax.fori_loop(0, local, load_second, 0)
    shared_loads[2].start()
    shared_loads[3].start()

    for load in small_loads:
        load.wait()
    lane_expert = lax.broadcasted_iota(jnp.int32, (experts, rows), 0)
    scale = jnp.zeros((experts, rows), f32)
    for k in range(ids.shape[0]):
        weight = weights[k : k + 1, :].astype(f32) * (1.0 / 64.0)
        scale = scale + jnp.where(ids[k : k + 1, :] == lane_expert, weight, 0.0)
    scales[z] = scale

    step = 16

    def norm(core):
        def body(t, carry):
            span = pl.ds(pl.multiple_of(core * share + t * step, step), step)
            value = blocks[z, span, :].astype(f32)
            square = jnp.sum(value * value, axis=1, keepdims=True)
            inverse = lax.rsqrt(square / width + EPSILON)
            blocks[z, span, :] = (value * inverse * gain[...]).astype(bf16)
            return carry

        lax.fori_loop(0, share // step, body, 0)

    def share_of(b):
        return blocks.at[b, pl.ds(0, share)]

    def piece_send(b, k, way):
        return pltpu.make_async_remote_copy(
            src_ref=blocks.at[b, rows_of(c, k)],
            dst_ref=blocks.at[b, rows_of(c, k)],
            send_sem=zsend.at[way, b],
            recv_sem=zrecv.at[b, k],
            device_id={"expert": lax.rem(z + (1 if way else owners - 1), owners)},
            device_id_type=MESH,
        )

    def scale_send(b, way):
        return pltpu.make_async_remote_copy(
            src_ref=scales.at[b],
            dst_ref=scales.at[b],
            send_sem=ssend.at[way, b],
            recv_sem=srecv.at[b],
            device_id={"expert": lax.rem(z + (1 if way else owners - 1), owners)},
            device_id_type=MESH,
        )

    pairs = groups // 2 if groups % 2 == 0 else groups
    lows = groups // pairs

    def mate(k, sign):
        high, low = k // lows, k % lows
        up = lax.rem(g // lows + (high if sign > 0 else pairs - high), pairs)
        return up * lows + lax.rem(lax.rem(g, lows) + (low if sign > 0 else lows - low), lows)

    def peer_rows(k, core):
        return pl.ds(pl.multiple_of((k - 1) * rows + core * share, share), share)

    def peer_send(k):
        mine = pl.ds(pl.multiple_of(c * share, share), share)
        return pltpu.make_async_remote_copy(
            src_ref=blocks.at[z, mine],
            dst_ref=peers.at[peer_rows(k, c)],
            send_sem=gsend,
            recv_sem=grecv.at[k - 1],
            device_id={"dp": mate(k, 1)},
            device_id_type=MESH,
        )

    def pass_piece(b, k, core):
        return pltpu.make_async_remote_copy(
            src_ref=blocks.at[b, rows_of(core, k)],
            dst_ref=blocks.at[b, rows_of(core, k)],
            send_sem=fsend.at[b],
            recv_sem=frecv.at[b],
            device_id={"tensor": other},
            device_id_type=MESH,
        )

    def pass_peer(k, core):
        return pltpu.make_async_remote_copy(
            src_ref=peers.at[peer_rows(k, core)],
            dst_ref=peers.at[peer_rows(k, core)],
            send_sem=psend,
            recv_sem=precv.at[k - 1],
            device_id={"tensor": other},
            device_id_type=MESH,
        )

    def exchange(i, p):
        at = pl.ds(*parts[p])
        turn = lax.rem(owners if isinstance(i, int) else i, 2)
        return pltpu.make_async_remote_copy(
            src_ref=staged.at[:, at],
            dst_ref=partner_routed.at[i, :, at],
            send_sem=esend.at[turn, p],
            recv_sem=erecv.at[turn, p],
            device_id={"tensor": other},
            device_id_type=MESH,
        )

    def result_send(i, p, slot, b):
        at = pl.ds(*parts[p])
        return pltpu.make_async_remote_copy(
            src_ref=partner_routed.at[i, :, at],
            dst_ref=landed.at[slot, :, at],
            send_sem=rsend.at[slot],
            recv_sem=rrecv.at[slot],
            device_id={"expert": b},
            device_id_type=MESH,
        )

    def relay_send(at):
        return pltpu.make_async_remote_copy(
            src_ref=partner_routed.at[last, :, pl.ds(*at)],
            dst_ref=relay.at[:, pl.ds(*at)],
            send_sem=nsend,
            recv_sem=nrecv.at[at[0] // TILE],
            device_id={"expert": jnp.where(z == 0, 1, owners - 2)},
            device_id_type=MESH,
        )

    def merged_send(at):
        return pltpu.make_async_remote_copy(
            src_ref=partner_routed.at[last, :, pl.ds(*at)],
            dst_ref=landed.at[jnp.where(z == 1, 1, owners - 3), :, pl.ds(*at)],
            send_sem=msend,
            recv_sem=mrecv.at[at[0] // TILE],
            device_id={"expert": jnp.where(z == 1, owners - 1, 0)},
            device_id_type=MESH,
        )

    def shared_exchange(j):
        return pltpu.make_async_remote_copy(
            src_ref=shared_staged.at[j - 1],
            dst_ref=partner_shared.at[j - 1],
            send_sem=xsend.at[j - 1],
            recv_sem=xrecv.at[j - 1],
            device_id={"tensor": other},
            device_id_type=MESH,
        )

    def shared_result(j):
        return pltpu.make_async_remote_copy(
            src_ref=partner_shared.at[j - 1],
            dst_ref=landed.at[owners - 1 + j - 1],
            send_sem=qsend,
            recv_sem=qrecv.at[j - 1],
            device_id={"dp": mate(j, -1)},
            device_id_type=MESH,
        )

    token_loads[0].wait()
    norm(c)
    pl.semaphore_wait(barrier, groups + 2 - at_end.astype(jnp.int32))

    def when(condition, action):
        @pl.when(condition)
        def _():
            action()

    def send_on(b, k, way):
        piece_send(b, k, way).start()
        if k == 0:
            scale_send(b, way).start()

    for k in range(PIECES):
        when(z + 1 < owners, lambda: send_on(z, k, 1))
        when(z > 0, lambda: send_on(z, k, 0))
    for k in range(1, groups):
        peer_send(k).start()

    token_loads[1].wait()
    norm(other)

    def arrive(b, k):
        here = blocks.at[b, rows_of(c, k)]
        pltpu.make_async_copy(here, here, zrecv.at[b, k]).wait()
        if k == 0:
            pltpu.make_async_copy(scales.at[b], scales.at[b], srecv.at[b]).wait()

    def fetch(d, k):
        @pl.when(z - d >= 0)
        def _():
            arrive(z - d, k)
            when(z + 1 < owners, lambda: send_on(z - d, k, 1))
            pass_piece(z - d, k, c).start()

        @pl.when(z + d < owners)
        def _():
            arrive(z + d, k)
            when(z > 0, lambda: send_on(z + d, k, 0))
            pass_piece(z + d, k, c).start()

    upper = z >= owners // 2
    near = jnp.where(upper, owners - 1 - z, z)

    def source(i):
        step_out = jnp.where(lax.rem(i, 2) == 1, near + lax.div(i + 1, 2), near - lax.div(i, 2))
        walk = jnp.where(i > 2 * near, i, step_out)
        return jnp.where(upper, owners - 1 - walk, walk)

    lane = lax.broadcasted_iota(jnp.int32, (rows, experts), 1)

    def expert(b, slot, e):
        both = dot(blocks[b], gate_up[e])
        column = jnp.transpose(scales[b])
        factor = jnp.sum(jnp.where(lane == z * local + e, column, 0.0), axis=1, keepdims=True)
        value = silu(both[:, 0:ff]) * both[:, ff:] * factor
        hidden[slot, :, pl.ds(pl.multiple_of(e * ff, LANES), ff)] = value.astype(bf16)

    own_shared = pl.ds((groups - 1) * rows, rows)

    def shared_first(span, block):
        both = dot(block, shared_in[...])
        shared_hidden[span] = (silu(both[:, 0:sff]) * both[:, sff:]).astype(bf16)

    early = max(local - 3, 0)
    hook = local * 3 // 4 - 1 if local > 1 else 0

    def own(e, carry):
        settle(gate_up.at[e], load_sem.at[e])
        expert(z, 0, e)
        when(e == early, lambda: fetch(1, 0))
        return carry

    lax.fori_loop(0, local, own, 0)
    settle(shared_in, shared_sem.at[0])
    shared_first(own_shared, blocks[z])
    for k in range(1, PIECES):
        fetch(1, k)

    def take_peer(k):
        here = peers.at[peer_rows(k, c)]
        pltpu.make_async_copy(here, here, grecv.at[k - 1]).wait()
        pass_peer(k, c).start()

    split = min(groups, 3)
    late, early_ones = range(1, split), range(split, groups)

    def take_peers(some):
        for k in some:
            take_peer(k)

    def shared_all(some):
        if not some:
            return
        if some is early_ones:
            settle(shared_out, shared_sem.at[1])
            take_peers(late)
        for j in some:
            pass_peer(j, other).wait_recv()
        span = pl.ds((some[0] - 1) * rows, len(some) * rows)
        shared_first(span, peers[span])
        value = dot(shared_hidden[span], shared_out[0])
        for n, j in enumerate(some):
            shared_staged[j - 1] = value[n * rows : (n + 1) * rows].astype(bf16)
            shared_exchange(j).start()

    def shared_rest(some):
        for j in some:
            shared_exchange(j).wait()
            value = dot(shared_hidden[pl.ds((j - 1) * rows, rows)], shared_out[1])
            partner_shared[j - 1] = (value + partner_shared[j - 1].astype(f32)).astype(bf16)
            shared_result(j).start()

    def direct(i):
        return (i < last) | jnp.logical_not(at_end | by_end) if merge else i > 0

    def send_result(i, p, slot, b):
        when(direct(i), lambda: result_send(i, p, slot, b).start())
        if merge:

            @pl.when((i == last) & at_end)
            def _():
                for at in tiles[p]:
                    relay_send(at).start()

    def routed(i, carry):
        b = source(i)
        settle(blocks.at[b, pl.ds(pl.multiple_of(other * share, share), share)], frecv.at[b])
        for e in range(local):
            expert(b, 1, e)
            if e == hook:
                when(i + 1 < owners, lambda: fetch(i + 1, 0))

        if owners > 2:
            when(i == 2, lambda: shared_rest(early_ones))

        @pl.when(i == 1)
        def _():
            for n in range(2):
                settle(down.at[n], down_sem.at[n])

        for p in range(len(parts)):
            at = pl.ds(*parts[p])
            staged[:, at] = dot(hidden[1], down[0, :, pl.ds(*parts[p])]).astype(bf16)
            exchange(i, p).start()
        for k in range(1, PIECES):
            when(i + 1 < owners, lambda: fetch(i + 1, k))
        when(i == 1, lambda: take_peers(early_ones))
        for p in range(len(parts)):
            keep[:, pl.ds(*parts[p])] = dot(hidden[1], down[1, :, pl.ds(*parts[p])])
        slot = lax.rem(z - b + owners, owners) - 1
        for p in range(len(parts)):
            at = pl.ds(*parts[p])
            exchange(i, p).wait()
            summed = keep[:, at] + partner_routed[i, :, at].astype(f32)
            partner_routed[i, :, at] = summed.astype(bf16)
            send_result(i, p, slot, b)
        when(i == 1, lambda: shared_all(early_ones))
        if owners == 2:
            shared_rest(early_ones)
        return carry

    lax.fori_loop(1, owners, routed, 0)

    shared_all(late)
    for p in range(len(parts)):
        at = pl.ds(*parts[p])
        value = dot(hidden[0], down[0, :, pl.ds(*parts[p])])
        value = value + dot(shared_hidden[own_shared], shared_out[0, :, pl.ds(*parts[p])])
        staged[:, at] = value.astype(bf16)
        exchange(0, p).start()
        if p == 0:
            shared_rest(late)

    every = sum(tiles, [])
    if merge:

        @pl.when(by_end)
        def _():
            for at in every:
                span = pl.ds(*at)
                pltpu.make_async_copy(relay.at[:, span], relay.at[:, span], nrecv.at[at[0] // TILE]).wait()
                value = partner_routed[last, :, span].astype(f32) + relay[:, span].astype(f32)
                partner_routed[last, :, span] = value.astype(bf16)
                merged_send(at).start()

    for p in range(len(parts)):
        value = dot(hidden[0], down[1, :, pl.ds(*parts[p])])
        keep[:, pl.ds(*parts[p])] = value + dot(shared_hidden[own_shared], shared_out[1, :, pl.ds(*parts[p])])
    for p in range(len(parts)):
        at = pl.ds(*parts[p])
        exchange(0, p).wait()
        keep[:, at] = keep[:, at] + partner_routed[0, :, at].astype(f32)

    def drained(i, carry):
        b = source(i)
        slot = lax.rem(z - b + owners, owners) - 1
        settle(share_of(b), fsend.at[b])

        def done():
            settle(landed.at[slot], rsend.at[slot])

        when(direct(i), done)
        return carry

    lax.fori_loop(1, owners, drained, 0)

    if merge:

        @pl.when(at_end)
        def _():
            settle(landed.at[0], nsend)

        @pl.when(by_end)
        def _():
            settle(landed.at[0], msend)

    def sent(b, carry):
        @pl.when((b <= z) & (z + 1 < owners))
        def _():
            settle(share_of(b), zsend.at[1, b])
            scale_send(b, 1).wait_send()

        @pl.when((b >= z) & (z > 0))
        def _():
            settle(share_of(b), zsend.at[0, b])
            scale_send(b, 0).wait_send()

        return carry

    lax.fori_loop(0, owners, sent, 0)
    for sem in (gsend, psend):
        settle(peers.at[pl.ds(0, (groups - 1) * share)], sem)
    settle(landed.at[pl.ds(0, groups - 1)], qsend)

    for j in range(1, groups):
        shared_result(j).wait_recv()
        keep[...] = keep[...] + landed[owners - 1 + j - 1].astype(f32)

    def gather(i, carry):
        slot = lax.rem(source(i) - z + owners, owners) - 1

        def arrived():
            settle(landed.at[slot], rrecv.at[slot])
            keep[...] = keep[...] + landed[slot].astype(f32)

        when((i < last - 1) | jnp.logical_not(at_end) if merge else i > 0, arrived)
        return carry

    lax.fori_loop(1, owners, gather, 0)
    if merge:

        @pl.when(at_end)
        def _():
            slot = jnp.where(z == 0, owners - 3, 1)
            for at in every:
                span = pl.ds(*at)
                here = landed.at[slot, :, span]
                pltpu.make_async_copy(here, here, mrecv.at[at[0] // TILE]).wait()
                keep[:, span] = keep[:, span] + landed[slot, :, span].astype(f32)

    out[...] = keep[...].astype(bf16)


def on_device(owners, groups, tokens, norm_gain, expert_ids, route_weights, *matrices):
    w_gate, w_up, w_down, shared_gate, shared_up, shared_down = matrices
    rows, width = tokens.shape
    half = width // 2
    local, ff, _ = w_down.shape
    sff = shared_down.shape[0]
    top = expert_ids.shape[1]
    tiles = -(-half // TILE)
    bf16, f32 = jnp.bfloat16, jnp.float32
    dma = pltpu.SemaphoreType.DMA
    anywhere = pl.BlockSpec(memory_space=pl.ANY)
    result = pl.pallas_call(
        functools.partial(kernel, owners, groups),
        out_shape=pltpu.VMEM((rows, half), bf16),
        in_specs=[anywhere] * 10,
        out_specs=pl.BlockSpec(memory_space=pltpu.VMEM),
        scratch_shapes=[
            pltpu.VMEM((owners, rows, width), bf16),
            pltpu.VMEM((owners, local * owners, rows), f32),
            pltpu.VMEM(((groups - 1) * rows, width), bf16),
            pltpu.VMEM((local, width, 2 * ff), bf16),
            pltpu.VMEM((2, local * ff, half), bf16),
            pltpu.VMEM((width, 2 * sff), bf16),
            pltpu.VMEM((2, sff, half), bf16),
            pltpu.VMEM((2, rows, local * ff), bf16),
            pltpu.VMEM((groups * rows, sff), bf16),
            pltpu.VMEM((rows, half), bf16),
            pltpu.VMEM((groups - 1, rows, half), bf16),
            pltpu.VMEM((rows, half), f32),
            pltpu.VMEM((rows, half), bf16),
            pltpu.VMEM((owners, rows, half), bf16),
            pltpu.VMEM((groups - 1, rows, half), bf16),
            pltpu.VMEM((owners + groups - 2, rows, half), bf16),
            pltpu.VMEM((1, width), f32),
            pltpu.VMEM((top, rows), jnp.int32),
            pltpu.VMEM((top, rows), jnp.int32),
            dma((local,)),
            dma((2,)),
            dma((2,)),
            dma((2,)),
            dma((3,)),
            dma((2, owners)),
            dma((owners, PIECES)),
            dma((2, owners)),
            dma((owners,)),
            dma(()),
            dma((groups - 1,)),
            dma((owners,)),
            dma((owners,)),
            dma(()),
            dma((groups - 1,)),
            dma((2, 2)),
            dma((2, 2)),
            dma((groups - 1,)),
            dma((groups - 1,)),
            dma((owners - 1,)),
            dma((owners - 1,)),
            dma(()),
            dma((groups - 1,)),
            dma(()),
            dma((tiles,)),
            dma(()),
            dma((tiles,)),
        ],
        compiler_params=pltpu.CompilerParams(
            collective_id=0, has_side_effects=True, vmem_limit_bytes=VMEM_BYTES
        ),
    )(tokens, norm_gain, expert_ids.T, route_weights.T, *matrices)
    return result


def solution(mesh):
    placed = (
        P(("dp", "expert"), None),
        P(),
        P(("dp", "expert"), None),
        P(("dp", "expert"), None),
        P("expert", None, "tensor"),
        P("expert", None, "tensor"),
        P("expert", "tensor", None),
        P(None, ("dp", "tensor")),
        P(None, ("dp", "tensor")),
        P(("dp", "tensor"), None),
    )
    return jax.shard_map(
        functools.partial(on_device, mesh.shape["expert"], mesh.shape["dp"]),
        mesh=mesh,
        in_specs=placed,
        out_specs=P(("dp", "expert"), "tensor"),
        check_vma=False,
    )
```

```python
import functools

import jax
import jax.numpy as jnp
from jax import lax
from jax.experimental import pallas as pl
from jax.experimental.pallas import tpu as pltpu
from jax.sharding import PartitionSpec as P

EPSILON = 1e-06
LANES = 128
PIECES = 2
TILE = 128
MESH = pl.DeviceIdType.MESH
VMEM_BYTES = 66400000


def dot(a, b):
    return jnp.dot(a, b, preferred_element_type=jnp.float32)


def silu(v):
    return v / (1.0 + jnp.exp(-v))


def kernel(
    owners,
    groups,
    tokens,
    gain_in,
    ids_in,
    weights_in,
    w_gate,
    w_up,
    w_down,
    shared_gate,
    shared_up,
    shared_down,
    out,
    blocks,
    scales,
    peers,
    gate_up,
    down,
    shared_in,
    shared_out,
    hidden,
    shared_hidden,
    staged,
    shared_staged,
    keep,
    relay,
    partner_routed,
    partner_shared,
    landed,
    gain,
    ids,
    weights,
    load_sem,
    down_sem,
    shared_sem,
    token_sem,
    small_sem,
    zsend,
    zrecv,
    ssend,
    srecv,
    gsend,
    grecv,
    fsend,
    frecv,
    psend,
    precv,
    esend,
    erecv,
    xsend,
    xrecv,
    rsend,
    rrecv,
    qsend,
    qrecv,
    msend,
    mrecv,
    nsend,
    nrecv,
):
    g = lax.axis_index("dp")
    z = lax.axis_index("expert")
    c = lax.axis_index("tensor")
    other = 1 - c
    local, ff, width = w_down.shape
    sff = shared_down.shape[0]
    rows = tokens.shape[0]
    half = width // 2
    experts = local * owners
    share = rows // 2
    piece = share // PIECES
    f32, bf16 = jnp.float32, jnp.bfloat16
    parts = ((0, half),)
    tiles = [
        [(at, min(TILE, first + size - at)) for at in range(first, first + size, TILE)]
        for first, size in parts
    ]
    merge = owners > 3
    at_end = (z == 0) | (z == owners - 1)
    by_end = (z == 1) | (z == owners - 2)
    last = owners - 1

    def rows_of(core, k):
        return pl.ds(pl.multiple_of(core * share + k * piece, piece), piece)

    token_loads = [
        pltpu.make_async_copy(
            tokens.at[pl.ds(pl.multiple_of(core * share, share), share)],
            blocks.at[z, pl.ds(pl.multiple_of(core * share, share), share)],
            token_sem.at[p],
        )
        for p, core in enumerate((c, other))
    ]
    small_loads = [
        pltpu.make_async_copy(gain_in, gain.at[0], small_sem.at[0]),
        pltpu.make_async_copy(ids_in, ids, small_sem.at[1]),
        pltpu.make_async_copy(weights_in, weights, small_sem.at[2]),
    ]
    barrier = pltpu.get_barrier_semaphore()
    for way in (1, owners - 1):

        @pl.when((z + 1 < owners) if way == 1 else (z > 0))
        def _():
            peer = {"expert": lax.rem(z + way, owners)}
            pl.semaphore_signal(barrier, inc=1, device_id=peer, device_id_type=MESH)

    for r in range(1, groups):
        peer = {"dp": lax.rem(g + r, groups)}
        pl.semaphore_signal(barrier, inc=1, device_id=peer, device_id_type=MESH)
    pl.semaphore_signal(barrier, inc=1, device_id={"tensor": other}, device_id_type=MESH)
    for load in token_loads + small_loads:
        load.start()

    def half_of(core):
        return pl.ds(pl.multiple_of(core * half, LANES), half)

    def settle(ref, sem):
        pltpu.make_async_copy(ref, ref, sem).wait()

    shared_loads = (
        pltpu.make_async_copy(shared_gate, shared_in.at[:, pl.ds(0, sff)], shared_sem.at[0]),
        pltpu.make_async_copy(shared_up, shared_in.at[:, pl.ds(sff, sff)], shared_sem.at[0]),
        pltpu.make_async_copy(shared_down.at[:, half_of(other)], shared_out.at[0], shared_sem.at[1]),
        pltpu.make_async_copy(shared_down.at[:, half_of(c)], shared_out.at[1], shared_sem.at[1]),
    )

    def load_first(e, carry):
        pltpu.make_async_copy(w_gate.at[e], gate_up.at[e, :, pl.ds(0, ff)], load_sem.at[e]).start()
        pltpu.make_async_copy(w_up.at[e], gate_up.at[e, :, pl.ds(ff, ff)], load_sem.at[e]).start()
        return carry

    def load_second(e, carry):
        first = pl.ds(pl.multiple_of(e * ff, LANES), ff)
        for n, core in enumerate((other, c)):
            part = w_down.at[e, :, half_of(core)]
            pltpu.make_async_copy(part, down.at[n, first], down_sem.at[n]).start()
        return carry

    lax.fori_loop(0, local - local // 4, load_first, 0)
    shared_loads[0].start()
    shared_loads[1].start()
    lax.fori_loop(local - local // 4, local, load_first, 0)
    lax.fori_loop(0, local, load_second, 0)
    shared_loads[2].start()
    shared_loads[3].start()

    for load in small_loads:
        load.wait()
    lane_expert = lax.broadcasted_iota(jnp.int32, (experts, rows), 0)
    scale = jnp.zeros((experts, rows), f32)
    for k in range(ids.shape[0]):
        weight = weights[k : k + 1, :].astype(f32) * (1.0 / 64.0)
        scale = scale + jnp.where(ids[k : k + 1, :] == lane_expert, weight, 0.0)
    scales[z] = scale

    step = 16

    def norm(core):
        def body(t, carry):
            span = pl.ds(pl.multiple_of(core * share + t * step, step), step)
            value = blocks[z, span, :].astype(f32)
            square = jnp.sum(value * value, axis=1, keepdims=True)
            inverse = lax.rsqrt(square / width + EPSILON)
            blocks[z, span, :] = (value * inverse * gain[...]).astype(bf16)
            return carry

        lax.fori_loop(0, share // step, body, 0)

    def share_of(b):
        return blocks.at[b, pl.ds(0, share)]

    def piece_send(b, k, way):
        return pltpu.make_async_remote_copy(
            src_ref=blocks.at[b, rows_of(c, k)],
            dst_ref=blocks.at[b, rows_of(c, k)],
            send_sem=zsend.at[way, b],
            recv_sem=zrecv.at[b, k],
            device_id={"expert": lax.rem(z + (1 if way else owners - 1), owners)},
            device_id_type=MESH,
        )

    def scale_send(b, way):
        return pltpu.make_async_remote_copy(
            src_ref=scales.at[b],
            dst_ref=scales.at[b],
            send_sem=ssend.at[way, b],
            recv_sem=srecv.at[b],
            device_id={"expert": lax.rem(z + (1 if way else owners - 1), owners)},
            device_id_type=MESH,
        )

    pairs = groups // 2 if groups % 2 == 0 else groups
    lows = groups // pairs

    def mate(k, sign):
        high, low = k // lows, k % lows
        up = lax.rem(g // lows + (high if sign > 0 else pairs - high), pairs)
        return up * lows + lax.rem(lax.rem(g, lows) + (low if sign > 0 else lows - low), lows)

    def peer_rows(k, core):
        return pl.ds(pl.multiple_of((k - 1) * rows + core * share, share), share)

    def peer_send(k):
        mine = pl.ds(pl.multiple_of(c * share, share), share)
        return pltpu.make_async_remote_copy(
            src_ref=blocks.at[z, mine],
            dst_ref=peers.at[peer_rows(k, c)],
            send_sem=gsend,
            recv_sem=grecv.at[k - 1],
            device_id={"dp": mate(k, 1)},
            device_id_type=MESH,
        )

    def pass_piece(b, k, core):
        return pltpu.make_async_remote_copy(
            src_ref=blocks.at[b, rows_of(core, k)],
            dst_ref=blocks.at[b, rows_of(core, k)],
            send_sem=fsend.at[b],
            recv_sem=frecv.at[b],
            device_id={"tensor": other},
            device_id_type=MESH,
        )

    def pass_peer(k, core):
        return pltpu.make_async_remote_copy(
            src_ref=peers.at[peer_rows(k, core)],
            dst_ref=peers.at[peer_rows(k, core)],
            send_sem=psend,
            recv_sem=precv.at[k - 1],
            device_id={"tensor": other},
            device_id_type=MESH,
        )

    def exchange(i, p):
        at = pl.ds(*parts[p])
        turn = lax.rem(owners if isinstance(i, int) else i, 2)
        return pltpu.make_async_remote_copy(
            src_ref=staged.at[:, at],
            dst_ref=partner_routed.at[i, :, at],
            send_sem=esend.at[turn, p],
            recv_sem=erecv.at[turn, p],
            device_id={"tensor": other},
            device_id_type=MESH,
        )

    def result_send(i, p, slot, b):
        at = pl.ds(*parts[p])
        return pltpu.make_async_remote_copy(
            src_ref=partner_routed.at[i, :, at],
            dst_ref=landed.at[slot, :, at],
            send_sem=rsend.at[slot],
            recv_sem=rrecv.at[slot],
            device_id={"expert": b},
            device_id_type=MESH,
        )

    def relay_send(at):
        return pltpu.make_async_remote_copy(
            src_ref=partner_routed.at[last, :, pl.ds(*at)],
            dst_ref=relay.at[:, pl.ds(*at)],
            send_sem=nsend,
            recv_sem=nrecv.at[at[0] // TILE],
            device_id={"expert": jnp.where(z == 0, 1, owners - 2)},
            device_id_type=MESH,
        )

    def merged_send(at):
        return pltpu.make_async_remote_copy(
            src_ref=partner_routed.at[last, :, pl.ds(*at)],
            dst_ref=landed.at[jnp.where(z == 1, 1, owners - 3), :, pl.ds(*at)],
            send_sem=msend,
            recv_sem=mrecv.at[at[0] // TILE],
            device_id={"expert": jnp.where(z == 1, owners - 1, 0)},
            device_id_type=MESH,
        )

    def shared_exchange(j):
        return pltpu.make_async_remote_copy(
            src_ref=shared_staged.at[j - 1],
            dst_ref=partner_shared.at[j - 1],
            send_sem=xsend.at[j - 1],
            recv_sem=xrecv.at[j - 1],
            device_id={"tensor": other},
            device_id_type=MESH,
        )

    def shared_result(j):
        return pltpu.make_async_remote_copy(
            src_ref=partner_shared.at[j - 1],
            dst_ref=landed.at[owners - 1 + j - 1],
            send_sem=qsend,
            recv_sem=qrecv.at[j - 1],
            device_id={"dp": mate(j, -1)},
            device_id_type=MESH,
        )

    token_loads[0].wait()
    norm(c)
    token_loads[1].wait()
    norm(other)
    pl.semaphore_wait(barrier, groups + 2 - at_end.astype(jnp.int32))

    def when(condition, action):
        @pl.when(condition)
        def _():
            action()

    def send_on(b, k, way):
        piece_send(b, k, way).start()
        if k == 0:
            scale_send(b, way).start()

    for k in range(PIECES):
        when(z + 1 < owners, lambda: send_on(z, k, 1))
        when(z > 0, lambda: send_on(z, k, 0))
    for k in range(1, groups):
        peer_send(k).start()


    def arrive(b, k):
        here = blocks.at[b, rows_of(c, k)]
        pltpu.make_async_copy(here, here, zrecv.at[b, k]).wait()
        if k == 0:
            pltpu.make_async_copy(scales.at[b], scales.at[b], srecv.at[b]).wait()

    def fetch(d, k):
        @pl.when(z - d >= 0)
        def _():
            arrive(z - d, k)
            when(z + 1 < owners, lambda: send_on(z - d, k, 1))
            pass_piece(z - d, k, c).start()

        @pl.when(z + d < owners)
        def _():
            arrive(z + d, k)
            when(z > 0, lambda: send_on(z + d, k, 0))
            pass_piece(z + d, k, c).start()

    upper = z >= owners // 2
    near = jnp.where(upper, owners - 1 - z, z)

    def source(i):
        step_out = jnp.where(lax.rem(i, 2) == 1, near + lax.div(i + 1, 2), near - lax.div(i, 2))
        walk = jnp.where(i > 2 * near, i, step_out)
        return jnp.where(upper, owners - 1 - walk, walk)

    lane = lax.broadcasted_iota(jnp.int32, (rows, experts), 1)

    def expert(b, slot, e):
        both = dot(blocks[b], gate_up[e])
        column = jnp.transpose(scales[b])
        factor = jnp.sum(jnp.where(lane == z * local + e, column, 0.0), axis=1, keepdims=True)
        value = silu(both[:, 0:ff]) * both[:, ff:] * factor
        hidden[slot, :, pl.ds(pl.multiple_of(e * ff, LANES), ff)] = value.astype(bf16)

    own_shared = pl.ds((groups - 1) * rows, rows)

    def shared_first(span, block):
        both = dot(block, shared_in[...])
        shared_hidden[span] = (silu(both[:, 0:sff]) * both[:, sff:]).astype(bf16)

    early = max(local - 3, 0)
    hook = local * 3 // 4 - 1 if local > 1 else 0

    def own(e, carry):
        settle(gate_up.at[e], load_sem.at[e])
        expert(z, 0, e)
        when(e == early, lambda: fetch(1, 0))
        return carry

    lax.fori_loop(0, local, own, 0)
    settle(shared_in, shared_sem.at[0])
    shared_first(own_shared, blocks[z])
    for k in range(1, PIECES):
        fetch(1, k)

    def take_peer(k):
        here = peers.at[peer_rows(k, c)]
        pltpu.make_async_copy(here, here, grecv.at[k - 1]).wait()
        pass_peer(k, c).start()

    split = min(groups, 3)
    late, early_ones = range(1, split), range(split, groups)

    def take_peers(some):
        for k in some:
            take_peer(k)

    def shared_all(some):
        if not some:
            return
        if some is early_ones:
            settle(shared_out, shared_sem.at[1])
            take_peers(late)
        for j in some:
            pass_peer(j, other).wait_recv()
        span = pl.ds((some[0] - 1) * rows, len(some) * rows)
        shared_first(span, peers[span])
        value = dot(shared_hidden[span], shared_out[0])
        for n, j in enumerate(some):
            shared_staged[j - 1] = value[n * rows : (n + 1) * rows].astype(bf16)
            shared_exchange(j).start()

    def shared_rest(some):
        for j in some:
            shared_exchange(j).wait()
            value = dot(shared_hidden[pl.ds((j - 1) * rows, rows)], shared_out[1])
            partner_shared[j - 1] = (value + partner_shared[j - 1].astype(f32)).astype(bf16)
            shared_result(j).start()

    def direct(i):
        return (i < last) | jnp.logical_not(at_end | by_end) if merge else i > 0

    def send_result(i, p, slot, b):
        when(direct(i), lambda: result_send(i, p, slot, b).start())
        if merge:

            @pl.when((i == last) & at_end)
            def _():
                for at in tiles[p]:
                    relay_send(at).start()

    turn = min(3, last)

    def routed(i, carry):
        b = source(i)
        settle(blocks.at[b, pl.ds(pl.multiple_of(other * share, share), share)], frecv.at[b])
        for e in range(local):
            expert(b, 1, e)
            if e == hook:
                when(i + 1 < owners, lambda: fetch(i + 1, 0))

        if owners > 2:
            when(i == turn, lambda: shared_rest(early_ones))

        @pl.when(i == 1)
        def _():
            for n in range(2):
                settle(down.at[n], down_sem.at[n])

        for p in range(len(parts)):
            at = pl.ds(*parts[p])
            staged[:, at] = dot(hidden[1], down[0, :, pl.ds(*parts[p])]).astype(bf16)
            exchange(i, p).start()
        for k in range(1, PIECES):
            when(i + 1 < owners, lambda: fetch(i + 1, k))
        when(i == 1, lambda: take_peers(early_ones))
        for p in range(len(parts)):
            keep[:, pl.ds(*parts[p])] = dot(hidden[1], down[1, :, pl.ds(*parts[p])])
        slot = lax.rem(z - b + owners, owners) - 1
        for p in range(len(parts)):
            at = pl.ds(*parts[p])
            exchange(i, p).wait()
            summed = keep[:, at] + partner_routed[i, :, at].astype(f32)
            partner_routed[i, :, at] = summed.astype(bf16)
            send_result(i, p, slot, b)
        when(i == turn - 1, lambda: shared_all(early_ones))
        if owners == 2:
            shared_rest(early_ones)
        return carry

    lax.fori_loop(1, owners, routed, 0)

    shared_all(late)
    for p in range(len(parts)):
        at = pl.ds(*parts[p])
        value = dot(hidden[0], down[0, :, pl.ds(*parts[p])])
        value = value + dot(shared_hidden[own_shared], shared_out[0, :, pl.ds(*parts[p])])
        staged[:, at] = value.astype(bf16)
        exchange(0, p).start()
        if p == 0:
            shared_rest(late)

    every = sum(tiles, [])
    if merge:

        @pl.when(by_end)
        def _():
            for at in every:
                span = pl.ds(*at)
                pltpu.make_async_copy(relay.at[:, span], relay.at[:, span], nrecv.at[at[0] // TILE]).wait()
                value = partner_routed[last, :, span].astype(f32) + relay[:, span].astype(f32)
                partner_routed[last, :, span] = value.astype(bf16)
                merged_send(at).start()

    for p in range(len(parts)):
        value = dot(hidden[0], down[1, :, pl.ds(*parts[p])])
        keep[:, pl.ds(*parts[p])] = value + dot(shared_hidden[own_shared], shared_out[1, :, pl.ds(*parts[p])])
    for p in range(len(parts)):
        at = pl.ds(*parts[p])
        exchange(0, p).wait()
        keep[:, at] = keep[:, at] + partner_routed[0, :, at].astype(f32)

    def drained(i, carry):
        b = source(i)
        slot = lax.rem(z - b + owners, owners) - 1
        settle(share_of(b), fsend.at[b])

        def done():
            settle(landed.at[slot], rsend.at[slot])

        when(direct(i), done)
        return carry

    lax.fori_loop(1, owners, drained, 0)

    if merge:

        @pl.when(at_end)
        def _():
            settle(landed.at[0], nsend)

        @pl.when(by_end)
        def _():
            settle(landed.at[0], msend)

    def sent(b, carry):
        @pl.when((b <= z) & (z + 1 < owners))
        def _():
            settle(share_of(b), zsend.at[1, b])
            scale_send(b, 1).wait_send()

        @pl.when((b >= z) & (z > 0))
        def _():
            settle(share_of(b), zsend.at[0, b])
            scale_send(b, 0).wait_send()

        return carry

    lax.fori_loop(0, owners, sent, 0)
    for sem in (gsend, psend):
        settle(peers.at[pl.ds(0, (groups - 1) * share)], sem)
    settle(landed.at[pl.ds(0, groups - 1)], qsend)

    for j in range(1, groups):
        shared_result(j).wait_recv()
        keep[...] = keep[...] + landed[owners - 1 + j - 1].astype(f32)

    def gather(i, carry):
        slot = lax.rem(source(i) - z + owners, owners) - 1

        def arrived():
            settle(landed.at[slot], rrecv.at[slot])
            keep[...] = keep[...] + landed[slot].astype(f32)

        when((i < last - 1) | jnp.logical_not(at_end) if merge else i > 0, arrived)
        return carry

    lax.fori_loop(1, owners, gather, 0)
    if merge:

        @pl.when(at_end)
        def _():
            slot = jnp.where(z == 0, owners - 3, 1)
            for at in every:
                span = pl.ds(*at)
                here = landed.at[slot, :, span]
                pltpu.make_async_copy(here, here, mrecv.at[at[0] // TILE]).wait()
                out[:, span] = (keep[:, span] + landed[slot, :, span].astype(f32)).astype(bf16)

    def plain():
        out[...] = keep[...].astype(bf16)

    when(jnp.logical_not(at_end) if merge else owners > 0, plain)


def on_device(owners, groups, tokens, norm_gain, expert_ids, route_weights, *matrices):
    w_gate, w_up, w_down, shared_gate, shared_up, shared_down = matrices
    rows, width = tokens.shape
    half = width // 2
    local, ff, _ = w_down.shape
    sff = shared_down.shape[0]
    top = expert_ids.shape[1]
    tiles = -(-half // TILE)
    bf16, f32 = jnp.bfloat16, jnp.float32
    dma = pltpu.SemaphoreType.DMA
    anywhere = pl.BlockSpec(memory_space=pl.ANY)
    result = pl.pallas_call(
        functools.partial(kernel, owners, groups),
        out_shape=pltpu.VMEM((rows, half), bf16),
        in_specs=[anywhere] * 10,
        out_specs=pl.BlockSpec(memory_space=pltpu.VMEM),
        scratch_shapes=[
            pltpu.VMEM((owners, rows, width), bf16),
            pltpu.VMEM((owners, local * owners, rows), f32),
            pltpu.VMEM(((groups - 1) * rows, width), bf16),
            pltpu.VMEM((local, width, 2 * ff), bf16),
            pltpu.VMEM((2, local * ff, half), bf16),
            pltpu.VMEM((width, 2 * sff), bf16),
            pltpu.VMEM((2, sff, half), bf16),
            pltpu.VMEM((2, rows, local * ff), bf16),
            pltpu.VMEM((groups * rows, sff), bf16),
            pltpu.VMEM((rows, half), bf16),
            pltpu.VMEM((groups - 1, rows, half), bf16),
            pltpu.VMEM((rows, half), f32),
            pltpu.VMEM((rows, half), bf16),
            pltpu.VMEM((owners, rows, half), bf16),
            pltpu.VMEM((groups - 1, rows, half), bf16),
            pltpu.VMEM((owners + groups - 2, rows, half), bf16),
            pltpu.VMEM((1, width), f32),
            pltpu.VMEM((top, rows), jnp.int32),
            pltpu.VMEM((top, rows), jnp.int32),
            dma((local,)),
            dma((2,)),
            dma((2,)),
            dma((2,)),
            dma((3,)),
            dma((2, owners)),
            dma((owners, PIECES)),
            dma((2, owners)),
            dma((owners,)),
            dma(()),
            dma((groups - 1,)),
            dma((owners,)),
            dma((owners,)),
            dma(()),
            dma((groups - 1,)),
            dma((2, 2)),
            dma((2, 2)),
            dma((groups - 1,)),
            dma((groups - 1,)),
            dma((owners - 1,)),
            dma((owners - 1,)),
            dma(()),
            dma((groups - 1,)),
            dma(()),
            dma((tiles,)),
            dma(()),
            dma((tiles,)),
        ],
        compiler_params=pltpu.CompilerParams(
            collective_id=0, has_side_effects=True, vmem_limit_bytes=VMEM_BYTES
        ),
    )(tokens, norm_gain, expert_ids.T, route_weights.T, *matrices)
    return result


def solution(mesh):
    placed = (
        P(("dp", "expert"), None),
        P(),
        P(("dp", "expert"), None),
        P(("dp", "expert"), None),
        P("expert", None, "tensor"),
        P("expert", None, "tensor"),
        P("expert", "tensor", None),
        P(None, ("dp", "tensor")),
        P(None, ("dp", "tensor")),
        P(("dp", "tensor"), None),
    )
    return jax.shard_map(
        functools.partial(on_device, mesh.shape["expert"], mesh.shape["dp"]),
        mesh=mesh,
        in_specs=placed,
        out_specs=P(("dp", "expert"), "tensor"),
        check_vma=False,
    )
```
